256 devices in a mesh: seq: 16 (over z, core), tp: 16 (over y, x).
Axes of the slice: x: 4, y: 4, z: 8, core: 2. Of those that a mesh axis runs over, the one named last changes fastest.
Arguments:
- latents: bfloat16 [16, 8192, 512], P(None, ('seq', 'tp')), may hold values from -6 to 6
- rotary_rows: bfloat16 [16, 8192, 64], P(None, ('seq', 'tp')), may hold values from -6 to 6
- latent_gain: float32 [512], replicated, may hold values from 0.25 to 1.75
- key_up: bfloat16 [512, 16, 128], P(None, 'tp'), may hold values from -0.25 to 0.25
- value_up: bfloat16 [512, 16, 128], P(None, 'tp'), may hold values from -0.25 to 0.25
Outputs:
- decode_keys: bfloat16 [16, 16, 192, 8192], P('seq', 'tp')
- decode_values: bfloat16 [16, 8192, 16, 128], P('seq', None, 'tp')
The draws below stay inside these ranges and needn't reach their ends.
All inputs are finite; a program needn't handle non-finite values.
Results may differ from the reference program's by a relative error of at most 0.0049.
Values may be sent and summed in bfloat16 or wider, within the bound.
No kernel may reach another device: no remote copies, remote signals or barrier semaphores. Data moves between devices by JAX's collectives and lax.ppermute only.
A program may use at most 64 MiB of HBM per device.

```python
import jax
import jax.numpy as jnp
from jax import lax

BATCH = 16
LENGTH = 8192
HEADS = 16
LATENT = 512
KEY_PART = 128
ROTARY = 64
VALUE_SIZE = 128


def levels(own_key, dims, shards, smallest, high):
    def one(dim, blocks):
        steps = jax.random.uniform(jax.random.fold_in(jax.random.fold_in(own_key, 6), dim), (blocks,), jnp.float32, smallest / len(shards), high / len(shards))
        return jnp.repeat(jnp.exp(steps), dims[dim] // blocks).reshape((-1,) + (1,) * (len(dims) - dim - 1))

    loudness = one(*shards[0])
    for cut in shards[1:]:
        loudness = loudness * one(*cut)
    return loudness


def bell_draw(rng, dims, width, limit, split=(), held_as=jnp.bfloat16):
    factor_of = levels(rng, dims, split, -0.22, 0.18) if split else 1.0
    array = jax.random.normal(rng, dims, jnp.float32) * width * factor_of
    return jnp.minimum(jnp.maximum(array, -limit), limit).astype(held_as)


def setup_inputs(seed: int = 0) -> dict:
    arg_keys = jax.random.split(jax.random.key(seed), 6)
    latents = bell_draw(arg_keys[0], (BATCH, LENGTH, LATENT), 1.0, 6.0, ((1, 256),))
    rotary_rows = bell_draw(arg_keys[1], (BATCH, LENGTH, ROTARY), 1.0, 6.0, ((1, 256),))
    latent_gain = jnp.clip(1.0 + 0.15 * jax.random.normal(arg_keys[2], (LATENT,), jnp.float32), 0.25, 1.75)
    key_up = bell_draw(arg_keys[3], (LATENT, HEADS, KEY_PART), LATENT ** -0.5, 0.25, ((1, 16),))
    value_up = bell_draw(arg_keys[4], (LATENT, HEADS, VALUE_SIZE), LATENT ** -0.5, 0.25, ((1, 16),))
    return dict(latents=latents, rotary_rows=rotary_rows, latent_gain=latent_gain, key_up=key_up, value_up=value_up)


def root_norm(vectors, row_gain):
    return vectors * lax.rsqrt(lax.optimization_barrier(jnp.mean(vectors * vectors, axis=-1, keepdims=True)) + 1e-06) * row_gain

def reference(latents, rotary_rows, latent_gain, key_up, value_up):
    rows_ready = root_norm(latents.astype(jnp.float32), latent_gain).astype(jnp.bfloat16)
    rows_ready = lax.optimization_barrier(rows_ready)

    def expand_one(one):
        rows_one, rotary_one = one
        wide_keys = jnp.einsum('tr,rhk->thk', rows_one.astype(jnp.float32), key_up.astype(jnp.float32)).astype(jnp.bfloat16)
        shared = jnp.broadcast_to(rotary_one[:, None], (LENGTH, HEADS, ROTARY))
        wide_values = jnp.einsum('tr,rhk->thk', rows_one.astype(jnp.float32), value_up.astype(jnp.float32)).astype(jnp.bfloat16)
        return (jnp.concatenate([wide_keys, shared], axis=-1), wide_values)
    decode_keys, decode_values = lax.map(expand_one, (rows_ready, rotary_rows))
    decode_keys = jnp.transpose(decode_keys, (0, 2, 3, 1))
    return (decode_keys, decode_values)
```

```python
import functools

import jax
import jax.numpy as jnp
from jax import lax
from jax.experimental import pallas as pl
from jax.experimental.pallas import tpu as pltpu
from jax.sharding import PartitionSpec as P


SIDE = 4
HOPS = (0, 1, -1, 2)
VMEM = pltpu.VMEM
MIB = 1 << 20


def move(array, along, hop):
    pairs = []
    for y in range(SIDE):
        for x in range(SIDE):
            to = (y, (x + hop) % SIDE) if along == "x" else ((y + hop) % SIDE, x)
            pairs.append((y * SIDE + x, to[0] * SIDE + to[1]))
    return lax.ppermute(array, "tp", pairs)


def whole(n):
    return [pl.BlockSpec(memory_space=VMEM)] * n


def cost(flops, nbytes):
    return pl.CostEstimate(flops=flops, bytes_accessed=nbytes, transcendentals=0)


def ready_kernel(lat, rot, gain, key_up, value_up, rows, weights):
    gains = gain[...]
    for b in range(lat.shape[0]):
        v = lat[b].astype(jnp.float32)
        v = v * lax.rsqrt(jnp.mean(v * v, axis=-1, keepdims=True) + 1e-06) * gains
        v = v.astype(jnp.bfloat16)
        for j in range(4):
            rows[b, 32 * j : 32 * j + 32, :] = v[:, 128 * j : 128 * j + 128]
        r = rot[b].astype(jnp.float32)
        rows[b, 128:144, :] = jnp.concatenate([r[:16], r[16:]], axis=-1).astype(jnp.bfloat16)
    weights[0:512, :] = key_up[...]
    weights[512:1024, :] = value_up[...]


def ready(latents, rotary, gain, key_up, value_up):
    batch = latents.shape[0]
    return pl.pallas_call(
        ready_kernel,
        out_shape=(
            jax.ShapeDtypeStruct((batch, 144, 128), jnp.bfloat16),
            jax.ShapeDtypeStruct((1024, 128), jnp.bfloat16),
        ),
        in_specs=whole(5),
        out_specs=tuple(whole(2)),
        compiler_params=pltpu.CompilerParams(vmem_limit_bytes=12 * MIB),
        cost_estimate=cost(4 * 512 * 512, 2 * MIB),
        name="ready",
    )(latents, rotary, gain.reshape(1, -1), key_up.reshape(512, 128), value_up.reshape(512, 128))


def expand_kernel(n_rows, n_heads, *refs):
    rows, heads, outs = refs[:n_rows], refs[n_rows : n_rows + n_heads], refs[n_rows + n_heads :]
    for h in range(n_heads):
        w = jnp.concatenate([heads[h][0:512, :], heads[h][512:1024, :]], axis=-1)
        for n in range(n_rows):
            a = rows[n]
            s = a.shape[0]
            lhs = jnp.concatenate(
                [a[:, 32 * j : 32 * j + 32, :].reshape(32 * s, 128) for j in range(4)], axis=-1
            )
            wide = jnp.dot(lhs, w, preferred_element_type=jnp.float32).astype(jnp.bfloat16)
            outs[h][n, :, 0:32, :] = wide[:, 0:128].reshape(s, 32, 128)
            outs[h][n, :, 32:64, :] = wide[:, 128:256].reshape(s, 32, 128)
            outs[h][n, :, 64:80, :] = a[:, 128:144, :]


def expand(rows, heads):
    n, s = len(rows), rows[0].shape[0]
    outs = pl.pallas_call(
        functools.partial(expand_kernel, n, len(heads)),
        out_shape=[jax.ShapeDtypeStruct((n, s, 80, 128), jnp.bfloat16)] * len(heads),
        in_specs=whole(n + len(heads)),
        out_specs=whole(len(heads)),
        compiler_params=pltpu.CompilerParams(vmem_limit_bytes=16 * MIB),
        cost_estimate=cost(n * s * 32 * 512 * 256 * 2 * len(heads), MIB),
        name="expand",
    )(*rows, *heads)
    return list(outs)


def swap_halves(v):
    return jnp.concatenate([v[:, 64:], v[:, :64]], axis=-1)


def join_kernel(outer_is_y, first, *refs):
    own, rest = refs[0:4], refs[4:8]
    keys, values, wide, turned = refs[-4:]
    t = lax.axis_index("tp")
    y, x = t // SIDE, t % SIDE
    g = pl.program_id(0)
    for half in range(2):
        s = 2 * g + half
        for o in range(4):
            for n in range(4):
                po, pn = (y, x) if outer_is_y else (x, y)
                po, pn = (po - HOPS[o] + SIDE) % SIDE, (pn - HOPS[n] + SIDE) % SIDE
                slot = po * SIDE + pn if outer_is_y else pn * SIDE + po
                src, at = (own[o], 0) if n == 0 else (rest[o], n - 1)
                to = pl.multiple_of(slot * 32, 32)
                wide[half, pl.ds(to, 32), :] = src[at, s, 0:32, :]
                values[pl.ds(pl.multiple_of(half * 512 + to, 32), 32), :] = src[at, s, 32:64, :]
                turned[half, pl.ds(pl.multiple_of(slot * 16, 16), 16), :] = src[at, s, 64:80, :]
    for part in range(4):
        lanes = slice(part * 128, part * 128 + 128)
        for half in range(2):
            block = slice(half * 512 + part * 128, half * 512 + part * 128 + 128)
            keys[0:128, block] = wide[half, lanes, :].T
        low = lax.broadcasted_iota(jnp.int32, (16, 128), 1) < 64
        pieces = []
        for q in range(4):
            at = (part * 4 + q) * 16
            a = turned[0, at : at + 16, :].astype(jnp.float32)
            b = turned[1, at : at + 16, :].astype(jnp.float32)
            pieces.append(jnp.where(low, a, swap_halves(b)))
            pieces.append(jnp.where(low, swap_halves(a), b))
        both = jnp.concatenate(pieces, axis=0).astype(jnp.bfloat16).T
        for half in range(2):
            block = slice(half * 512 + part * 128, half * 512 + part * 128 + 128)
            keys[128:192, block] = both[64 * half : 64 * half + 64, :]


def join(own, rest, outer_is_y, first, before=None):
    steps = own[0].shape[1] // 2
    aliased = [] if before is None else list(before)
    n = len(own) + len(rest)
    return pl.pallas_call(
        functools.partial(join_kernel, outer_is_y, first),
        grid=(steps,),
        out_shape=(
            jax.ShapeDtypeStruct((192, 8192), jnp.bfloat16),
            jax.ShapeDtypeStruct((8192, 128), jnp.bfloat16),
        ),
        in_specs=whole(n) + [pl.BlockSpec(memory_space=pl.ANY)] * len(aliased),
        out_specs=(
            pl.BlockSpec((192, 1024), lambda g: (0, g + first)),
            pl.BlockSpec((1024, 128), lambda g: (g + first, 0)),
        ),
        scratch_shapes=[VMEM((2, 512, 128), jnp.bfloat16), VMEM((2, 256, 128), jnp.bfloat16)],
        input_output_aliases={n + i: i for i in range(len(aliased))},
        compiler_params=pltpu.CompilerParams(vmem_limit_bytes=20 * MIB),
        cost_estimate=cost(0, 8 * MIB),
        name="join",
    )(*own, *rest, *aliased)


def shards(latents, rotary_rows, latent_gain, key_up, value_up):
    rows, head = ready(latents, rotary_rows, latent_gain, key_up, value_up)
    mine = lax.all_to_all(rows, "seq", split_axis=0, concat_axis=0, tiled=True)
    heads = {
        axis: [head] + [move(head, axis, -hop) for hop in HOPS[1:]] for axis in "yx"
    }
    half = mine.shape[0] // 2
    halves = {"x": mine[:half], "y": mine[half:]}
    other = {"x": "y", "y": "x"}
    near = {a: [move(halves[a], a, hop) for hop in HOPS[1:]] for a in "xy"}
    own_out, rest_out = {}, {}
    for a in "xy":
        own_out[a] = expand([halves[a]], heads[other[a]])
        own_out[a] = own_out[a][:1] + [
            move(p, other[a], hop) for p, hop in zip(own_out[a][1:], HOPS[1:])
        ]
    for a in "xy":
        rest_out[a] = [None] * 4
    for i in (3, 1, 2, 0):
        for a in "xy":
            (piece,) = expand(near[a], [heads[other[a]][i]])
            rest_out[a][i] = move(piece, other[a], HOPS[i]) if i else piece
    outs = join(own_out["x"], rest_out["x"], True, 0)
    keys, values = join(own_out["y"], rest_out["y"], False, half // 2, outs)
    return keys[None, None], values[None, :, None, :]


def solution(mesh):
    return jax.shard_map(
        shards,
        mesh=mesh,
        in_specs=(
            P(None, ("seq", "tp"), None),
            P(None, ("seq", "tp"), None),
            P(),
            P(None, "tp", None),
            P(None, "tp", None),
        ),
        out_specs=(P("seq", "tp", None, None), P("seq", None, "tp", None)),
        check_vma=False,
    )
```

```python
import functools

import jax
import jax.numpy as jnp
from jax import lax
from jax.experimental import pallas as pl
from jax.experimental.pallas import tpu as pltpu
from jax.sharding import PartitionSpec as P


SIDE = 4
HOPS = (0, 1, -1, 2)
VMEM = pltpu.VMEM
MIB = 1 << 20


def move(array, along, hop):
    pairs = []
    for y in range(SIDE):
        for x in range(SIDE):
            to = (y, (x + hop) % SIDE) if along == "x" else ((y + hop) % SIDE, x)
            pairs.append((y * SIDE + x, to[0] * SIDE + to[1]))
    return lax.ppermute(array, "tp", pairs)


def whole(n):
    return [pl.BlockSpec(memory_space=VMEM)] * n


def cost(flops, nbytes):
    return pl.CostEstimate(flops=flops, bytes_accessed=nbytes, transcendentals=0)


def ready_kernel(lat_in, rot_in, gain_in, key_in, value_in, rows, weights, lat, rot, gain, sems):
    copies = [
        pltpu.make_async_copy(src, dst, sems.at[i])
        for i, (src, dst) in enumerate(
            (
                (lat_in, lat),
                (gain_in, gain),
                (rot_in, rot),
                (key_in, weights.at[0:512, :]),
                (value_in, weights.at[512:1024, :]),
            )
        )
    ]
    for copy in copies:
        copy.start()
    copies[0].wait()
    copies[1].wait()
    gains = gain[...]
    for b in range(lat.shape[0]):
        v = lat[b].astype(jnp.float32)
        v = v * lax.rsqrt(jnp.mean(v * v, axis=-1, keepdims=True) + 1e-06) * gains
        v = v.astype(jnp.bfloat16)
        for j in range(4):
            rows[b, 32 * j : 32 * j + 32, :] = v[:, 128 * j : 128 * j + 128]
    copies[2].wait()
    for b in range(lat.shape[0]):
        r = rot[b].astype(jnp.float32)
        rows[b, 128:144, :] = jnp.concatenate([r[:16], r[16:]], axis=-1).astype(jnp.bfloat16)
    copies[3].wait()
    copies[4].wait()


def ready(latents, rotary, gain, key_up, value_up):
    batch = latents.shape[0]
    return pl.pallas_call(
        ready_kernel,
        out_shape=(
            jax.ShapeDtypeStruct((batch, 144, 128), jnp.bfloat16),
            jax.ShapeDtypeStruct((1024, 128), jnp.bfloat16),
        ),
        in_specs=[pl.BlockSpec(memory_space=pltpu.HBM)] * 5,
        out_specs=tuple(whole(2)),
        scratch_shapes=[
            VMEM(latents.shape, jnp.bfloat16),
            VMEM(rotary.shape, jnp.bfloat16),
            VMEM((1, 512), jnp.float32),
            pltpu.SemaphoreType.DMA((5,)),
        ],
        compiler_params=pltpu.CompilerParams(vmem_limit_bytes=67043328),
        cost_estimate=cost(4 * 512 * 512, 2 * MIB),
        name="ready",
    )(latents, rotary, gain.reshape(1, -1), key_up.reshape(512, 128), value_up.reshape(512, 128))


def expand_kernel(n_rows, n_heads, *refs):
    rows, heads, outs = refs[:n_rows], refs[n_rows : n_rows + n_heads], refs[n_rows + n_heads :]
    for h in range(n_heads):
        w = jnp.concatenate([heads[h][0:512, :], heads[h][512:1024, :]], axis=-1)
        for n in range(n_rows):
            a = rows[n]
            s = a.shape[0]
            lhs = jnp.concatenate(
                [a[:, 32 * j : 32 * j + 32, :].reshape(32 * s, 128) for j in range(4)], axis=-1
            )
            wide = jnp.dot(lhs, w, preferred_element_type=jnp.float32).astype(jnp.bfloat16)
            outs[h][n, :, 0:32, :] = wide[:, 0:128].reshape(s, 32, 128)
            outs[h][n, :, 32:64, :] = wide[:, 128:256].reshape(s, 32, 128)
            outs[h][n, :, 64:80, :] = a[:, 128:144, :]


def expand(rows, heads):
    n, s = len(rows), rows[0].shape[0]
    outs = pl.pallas_call(
        functools.partial(expand_kernel, n, len(heads)),
        out_shape=[jax.ShapeDtypeStruct((n, s, 80, 128), jnp.bfloat16)] * len(heads),
        in_specs=whole(n + len(heads)),
        out_specs=whole(len(heads)),
        compiler_params=pltpu.CompilerParams(vmem_limit_bytes=16 * MIB),
        cost_estimate=cost(n * s * 32 * 512 * 256 * 2 * len(heads), MIB),
        name="expand",
    )(*rows, *heads)
    return list(outs)


def swap_halves(v):
    return jnp.concatenate([v[:, 64:], v[:, :64]], axis=-1)


def join_kernel(outer_is_y, *refs):
    own, rest = refs[0:4], refs[4:8]
    keys, values, wide, turned = refs[-4:]
    t = lax.axis_index("tp")
    y, x = t // SIDE, t % SIDE
    g = pl.program_id(0)
    for half in range(2):
        s = 2 * g + half
        for o in range(4):
            for n in range(4):
                po, pn = (y, x) if outer_is_y else (x, y)
                po, pn = (po - HOPS[o] + SIDE) % SIDE, (pn - HOPS[n] + SIDE) % SIDE
                slot = po * SIDE + pn if outer_is_y else pn * SIDE + po
                src, at = (own[o], 0) if n == 0 else (rest[o], n - 1)
                to = pl.multiple_of(slot * 32, 32)
                wide[half, pl.ds(to, 32), :] = src[at, s, 0:32, :]
                values[pl.ds(pl.multiple_of(half * 512 + to, 32), 32), :] = src[at, s, 32:64, :]
                turned[half, pl.ds(pl.multiple_of(slot * 16, 16), 16), :] = src[at, s, 64:80, :]
    for part in range(4):
        lanes = slice(part * 128, part * 128 + 128)
        for half in range(2):
            block = slice(half * 512 + part * 128, half * 512 + part * 128 + 128)
            keys[0:128, block] = wide[half, lanes, :].T
        low = lax.broadcasted_iota(jnp.int32, (16, 128), 1) < 64
        pieces = []
        for q in range(4):
            at = (part * 4 + q) * 16
            a = turned[0, at : at + 16, :].astype(jnp.float32)
            b = turned[1, at : at + 16, :].astype(jnp.float32)
            pieces.append(jnp.where(low, a, swap_halves(b)))
            pieces.append(jnp.where(low, swap_halves(a), b))
        both = jnp.concatenate(pieces, axis=0).astype(jnp.bfloat16).T
        for half in range(2):
            block = slice(half * 512 + part * 128, half * 512 + part * 128 + 128)
            keys[128:192, block] = both[64 * half : 64 * half + 64, :]


def join(own, rest, outer_is_y, first, before=None):
    steps = own[0].shape[1] // 2
    aliased = [] if before is None else list(before)
    n = len(own) + len(rest)
    return pl.pallas_call(
        functools.partial(join_kernel, outer_is_y),
        grid=(steps,),
        out_shape=(
            jax.ShapeDtypeStruct((192, 8192), jnp.bfloat16),
            jax.ShapeDtypeStruct((8192, 128), jnp.bfloat16),
        ),
        in_specs=whole(n) + [pl.BlockSpec(memory_space=pl.ANY)] * len(aliased),
        out_specs=(
            pl.BlockSpec((192, 1024), lambda g: (0, g + first)),
            pl.BlockSpec((1024, 128), lambda g: (g + first, 0)),
        ),
        scratch_shapes=[VMEM((2, 512, 128), jnp.bfloat16), VMEM((2, 256, 128), jnp.bfloat16)],
        input_output_aliases={n + i: i for i in range(len(aliased))},
        compiler_params=pltpu.CompilerParams(vmem_limit_bytes=20 * MIB),
        cost_estimate=cost(0, 8 * MIB),
        name="join",
    )(*own, *rest, *aliased)


def shards(latents, rotary_rows, latent_gain, key_up, value_up):
    rows, head = ready(latents, rotary_rows, latent_gain, key_up, value_up)
    heads = {
        axis: [head] + [move(head, axis, -hop) for hop in HOPS[1:]] for axis in "yx"
    }
    mine = lax.all_to_all(rows, "seq", split_axis=0, concat_axis=0, tiled=True)
    mine, heads = lax.optimization_barrier((mine, heads))
    half = mine.shape[0] // 2
    halves = {"x": mine[:half], "y": mine[half:]}
    other = {"x": "y", "y": "x"}
    near = {"x": [], "y": []}
    own_out = {"x": [None] * 4, "y": [None] * 4}
    rest_out = {"x": [None] * 4, "y": [None] * 4}
    for i in (1, 2, 3):
        for a in "xy":
            near[a].append(move(halves[a], a, HOPS[i]))
    for a in "xy":
        own_out[a] = expand([halves[a]], heads[other[a]])
    for i in (3, 1, 2):
        for a in "xy":
            own_out[a][i] = move(own_out[a][i], other[a], HOPS[i])
    for i in (3, 1, 2, 0):
        for a in "xy":
            (piece,) = expand(near[a], [heads[other[a]][i]])
            rest_out[a][i] = move(piece, other[a], HOPS[i]) if i else piece
    outs = join(own_out["x"], rest_out["x"], True, 0)
    keys, values = join(own_out["y"], rest_out["y"], False, half // 2, outs)
    return keys[None, None], values[None, :, None, :]


def solution(mesh):
    return jax.shard_map(
        shards,
        mesh=mesh,
        in_specs=(
            P(None, ("seq", "tp"), None),
            P(None, ("seq", "tp"), None),
            P(),
            P(None, "tp", None),
            P(None, "tp", None),
        ),
        out_specs=(P("seq", "tp", None, None), P("seq", None, "tp", None)),
        check_vma=False,
    )
```

```python
import functools

import jax
import jax.numpy as jnp
from jax import lax
from jax.experimental import pallas as pl
from jax.experimental.pallas import tpu as pltpu
from jax.sharding import PartitionSpec as P


SIDE = 4
HOPS = (0, 1, -1, 2)
VMEM = pltpu.VMEM
MIB = 1 << 20
BF16 = jnp.bfloat16
OTHER = {"x": "y", "y": "x"}


def move(array, along, hop):
    pairs = []
    for y in range(SIDE):
        for x in range(SIDE):
            to = (y, (x + hop) % SIDE) if along == "x" else ((y + hop) % SIDE, x)
            pairs.append((y * SIDE + x, to[0] * SIDE + to[1]))
    return lax.ppermute(array, "tp", pairs)


def sender(along, hop):
    t = lax.axis_index("tp")
    mine = t % SIDE if along == "x" else t // SIDE
    return (mine - hop + SIDE) % SIDE


def whole(n, space=VMEM):
    return [pl.BlockSpec(memory_space=space)] * n


def shape(*dims):
    return jax.ShapeDtypeStruct(dims, BF16)


def call(kernel, outs, args, out_space=VMEM, in_specs=None, limit=24 * MIB, scratch=(), alias=None, flops=0, nbytes=MIB):
    return pl.pallas_call(
        kernel,
        out_shape=outs,
        in_specs=in_specs or whole(len(args)),
        out_specs=jax.tree.map(lambda _: pl.BlockSpec(memory_space=out_space), outs),
        scratch_shapes=list(scratch),
        input_output_aliases=alias or {},
        compiler_params=pltpu.CompilerParams(vmem_limit_bytes=limit),
        cost_estimate=pl.CostEstimate(flops=flops, bytes_accessed=nbytes, transcendentals=0),
    )(*args)


def run_all(copies):
    for copy in copies:
        copy.start()
    for copy in copies:
        copy.wait()


def pack_kernel(rot_in, key_in, value_in, rotary, weights, rot, sems):
    copies = [
        pltpu.make_async_copy(rot_in, rot, sems.at[0]),
        pltpu.make_async_copy(key_in, weights.at[0:512, :], sems.at[1]),
        pltpu.make_async_copy(value_in, weights.at[512:1024, :], sems.at[2]),
    ]
    for copy in copies:
        copy.start()
    copies[0].wait()
    pairs = rot.shape[0] // 2
    for b in range(pairs):
        both = [rot[b].astype(jnp.float32), rot[b + pairs].astype(jnp.float32)]
        rotary[b] = jnp.concatenate(both, axis=-1).astype(BF16)
    copies[1].wait()
    copies[2].wait()


def pack(rotary, key_up, value_up):
    b = rotary.shape[0]
    return call(
        pack_kernel,
        (shape(b // 2, 32, 128), shape(1024, 128)),
        (rotary, key_up.reshape(512, 128), value_up.reshape(512, 128)),
        in_specs=whole(3, pltpu.HBM),
        limit=67043328,
        scratch=[VMEM(rotary.shape, BF16), pltpu.SemaphoreType.DMA((3,))],
    )


def rotary_row_kernel(*refs):
    got, out, block = refs[:4], refs[4], refs[5]
    pairs = got[0].shape[0]
    for i, hop in enumerate(HOPS):
        at = pl.multiple_of(sender("x", hop) * 32, 32)
        for b in range(pairs):
            block[b, pl.ds(at, 32), :] = got[i][b]
    for b in range(pairs):
        turned = block[b].T
        out[b] = turned[0:64]
        out[b + pairs] = turned[64:128]


def rotary_row(got):
    pairs = got[0].shape[0]
    return call(
        rotary_row_kernel,
        shape(2 * pairs, 64, 128),
        got,
        limit=4 * MIB,
        scratch=[VMEM((pairs, 128, 128), BF16)],
    )


def rotary_plane_kernel(*refs):
    got, out = refs[:4], refs[4]
    for i, hop in enumerate(HOPS):
        out[:, pl.ds(sender("y", hop), 1), :, :] = got[i][...][:, None]


def rotary_plane(got):
    return call(rotary_plane_kernel, shape(got[0].shape[0], SIDE, 64, 128), got, limit=4 * MIB)


def norm_kernel(rows, gain, low, high):
    gains = gain[...]
    half = low.shape[0]
    for b in range(rows.shape[0]):
        v = rows[b].astype(jnp.float32)
        v = v * lax.rsqrt(jnp.mean(v * v, axis=-1, keepdims=True) + 1e-06) * gains
        (low if b < half else high)[b % half] = v.astype(BF16)


def norm(rows, gain):
    n = rows.shape[0]
    outs = (shape(n // 2, 32, 512),) * 2
    return call(norm_kernel, outs, (rows, gain.reshape(1, -1)), limit=4 * MIB)


def expand_kernel(along, *refs):
    rows, head, out, block = refs[:4], refs[4], refs[5], refs[6]
    s = block.shape[0]
    for i, hop in enumerate(HOPS):
        at = pl.multiple_of(sender(along, hop) * 32, 32)
        for b in range(s):
            block[b, pl.ds(at, 32), :] = rows[i][b]
    w = jnp.concatenate([head[0:512, :], head[512:1024, :]], axis=-1)
    for b in range(0, s, 2):
        wide = jnp.dot(
            block[b : b + 2].reshape(256, 512), w, preferred_element_type=jnp.float32
        ).astype(BF16)
        for k in range(2):
            part = wide[128 * k : 128 * k + 128]
            out[b + k, 0] = part[:, 0:128].T
            out[b + k, 1] = part[:, 128:256]


def expand(rows, head, along):
    s = rows[0].shape[0]
    return call(
        functools.partial(expand_kernel, along),
        shape(s, 2, 128, 128),
        (*rows, head),
        limit=8 * MIB,
        scratch=[VMEM((s, 128, 512), BF16)],
        flops=s * 128 * 512 * 256 * 2,
    )


def join_x_kernel(first, *refs):
    got, keys, values, sems = refs[:4], refs[-3], refs[-2], refs[-1]
    s = got[0].shape[0]
    copies = []
    for i, hop in enumerate(HOPS):
        y = sender("y", hop)
        sem = lambda: sems.at[len(copies)]
        copies.append(pltpu.make_async_copy(got[i].at[:, 1], values.at[first : first + s, y], sem()))
        for b in range(s):
            lanes = pl.ds(pl.multiple_of((first + b) * 512 + y * 128, 128), 128)
            copies.append(pltpu.make_async_copy(got[i].at[b, 0], keys.at[0:128, lanes], sem()))
    run_all(copies)


def join_y_kernel(first, *refs):
    got, keys, values, sorted_, lined, sems = refs[:4], *refs[-5:]
    s = got[0].shape[0]
    copies = []
    sem = lambda: sems.at[len(copies)]
    for i, hop in enumerate(HOPS):
        x = sender("x", hop)
        rows = pl.ds(pl.multiple_of(x * 32, 32), 32)
        for y in range(SIDE):
            copies.append(
                pltpu.make_async_copy(
                    got[i].at[:, 1, 32 * y : 32 * y + 32],
                    values.at[first : first + s, y, rows],
                    sem(),
                )
            )
    for copy in copies:
        copy.start()
    for i, hop in enumerate(HOPS):
        x = sender("x", hop)
        for b in range(s):
            sorted_[x, b] = got[i][b, 0]
    for b in range(s):
        for y in range(SIDE):
            parts = [sorted_[x, b][:, 32 * y : 32 * y + 32] for x in range(SIDE)]
            lined[b, :, 128 * y : 128 * y + 128] = jnp.concatenate(parts, axis=-1)
        at = (first + b) * 512
        copies.append(pltpu.make_async_copy(lined.at[b], keys.at[0:128, at : at + 512], sem()))
        copies[-1].start()
    for copy in copies:
        copy.wait()


def join_rotary_kernel(got, keys_in, keys, sems):
    del keys_in
    copies = []
    for b in range(got.shape[0]):
        for y in range(SIDE):
            at = b * 512 + y * 128
            copies.append(
                pltpu.make_async_copy(
                    got.at[b, y], keys.at[128:192, at : at + 128], sems.at[len(copies)]
                )
            )
    run_all(copies)


def joins(x_got, y_got, rotary):
    n = rotary.shape[0]
    s = n // 2
    outs = (shape(192, n * 512), shape(n, SIDE, 128, 128))
    sems = lambda k: pltpu.SemaphoreType.DMA((k,))
    keys, values = call(
        functools.partial(join_x_kernel, 0),
        outs,
        x_got,
        out_space=pltpu.HBM,
        limit=8 * MIB,
        scratch=[sems(SIDE * (s + 1))],
        nbytes=4 * MIB,
    )
    keys, values = call(
        functools.partial(join_y_kernel, s),
        outs,
        (*y_got, keys, values),
        out_space=pltpu.HBM,
        in_specs=whole(4) + whole(2, pltpu.HBM),
        limit=8 * MIB,
        scratch=[
            VMEM((SIDE, s, 128, 128), BF16),
            VMEM((s, 128, 512), BF16),
            sems(SIDE * SIDE + s),
        ],
        alias={4: 0, 5: 1},
        nbytes=4 * MIB,
    )
    keys = call(
        join_rotary_kernel,
        outs[0],
        (rotary, keys),
        out_space=pltpu.HBM,
        in_specs=whole(1) + whole(1, pltpu.HBM),
        limit=4 * MIB,
        scratch=[sems(n * SIDE)],
        alias={1: 0},
        nbytes=2 * MIB,
    )
    return keys, values


def named_move(array, along, i, back=False):
    return move(array, along, -HOPS[i] if back else HOPS[i])


def shards(latents, rotary_rows, latent_gain, key_up, value_up):
    mine = lax.all_to_all(latents, "seq", split_axis=0, concat_axis=0, tiled=True)
    rotary, head = pack(rotary_rows, key_up, value_up)
    row = rotary_row([rotary] + [named_move(rotary, "x", i) for i in (1, 2, 3)])
    plane = [row] + [named_move(row, "y", i) for i in (1, 2, 3)]
    heads = {a: [head] + [named_move(head, a, i, back=True) for i in (1, 2, 3)] for a in "xy"}
    mine, _ = lax.optimization_barrier((mine, row))
    halves = dict(zip("xy", norm(mine, latent_gain)))
    near = {a: [halves[a]] for a in "xy"}
    for i in (1, 2, 3):
        for a in "xy":
            near[a].append(named_move(halves[a], a, i))
    plane = rotary_plane(plane)
    far = lax.all_to_all(plane, "seq", split_axis=0, concat_axis=0, tiled=True)
    got = {"x": [None] * 4, "y": [None] * 4}
    for i in (3, 1, 2, 0):
        for a in "xy":
            piece = expand(near[a], heads[OTHER[a]][i], a)
            got[a][i] = named_move(piece, OTHER[a], i) if i else piece
    keys, values = joins(got["x"], got["y"], far)
    return keys[None, None], values.reshape(1, -1, 1, 128)


def solution(mesh):
    return jax.shard_map(
        shards,
        mesh=mesh,
        in_specs=(
            P(None, ("seq", "tp"), None),
            P(None, ("seq", "tp"), None),
            P(),
            P(None, "tp", None),
            P(None, "tp", None),
        ),
        out_specs=(P("seq", "tp", None, None), P("seq", None, "tp", None)),
        check_vma=False,
    )
```

```python
import functools

import jax
import jax.numpy as jnp
from jax import lax
from jax.experimental import pallas as pl
from jax.experimental.pallas import tpu as pltpu
from jax.sharding import PartitionSpec as P


SIDE = 4
HOPS = (0, 1, -1, 2)
VMEM = pltpu.VMEM
MIB = 1 << 20
BF16 = jnp.bfloat16
OTHER = {"x": "y", "y": "x"}


def move(array, along, hop):
    pairs = []
    for y in range(SIDE):
        for x in range(SIDE):
            to = (y, (x + hop) % SIDE) if along == "x" else ((y + hop) % SIDE, x)
            pairs.append((y * SIDE + x, to[0] * SIDE + to[1]))
    return lax.ppermute(array, "tp", pairs)


def sender(along, hop):
    t = lax.axis_index("tp")
    mine = t % SIDE if along == "x" else t // SIDE
    return (mine - hop + SIDE) % SIDE


def whole(n, space=VMEM):
    return [pl.BlockSpec(memory_space=space)] * n


def shape(*dims):
    return jax.ShapeDtypeStruct(dims, BF16)


def call(kernel, outs, args, out_space=VMEM, in_specs=None, limit=24 * MIB, scratch=(), alias=None, flops=0, nbytes=MIB):
    return pl.pallas_call(
        kernel,
        out_shape=outs,
        in_specs=in_specs or whole(len(args)),
        out_specs=jax.tree.map(lambda _: pl.BlockSpec(memory_space=out_space), outs),
        scratch_shapes=list(scratch),
        input_output_aliases=alias or {},
        compiler_params=pltpu.CompilerParams(vmem_limit_bytes=limit),
        cost_estimate=pl.CostEstimate(flops=flops, bytes_accessed=nbytes, transcendentals=0),
    )(*args)


def regroup(parts):
    return [jnp.concatenate([p[:, 32 * k : 32 * k + 32] for p in parts], axis=-1) for k in range(4)]


def ready_kernel(lat_in, rot_in, gain_in, key_in, value_in, rows, weights, lat, rot, gain, sems):
    copies = [
        pltpu.make_async_copy(src, dst, sems.at[i])
        for i, (src, dst) in enumerate(
            (
                (lat_in, lat),
                (gain_in, gain),
                (rot_in, rot),
                (key_in, weights.at[0:512, :]),
                (value_in, weights.at[512:1024, :]),
            )
        )
    ]
    for copy in copies:
        copy.start()
    copies[0].wait()
    copies[1].wait()
    gains = gain[...]
    for b in range(lat.shape[0]):
        v = lat[b].astype(jnp.float32)
        v = v * lax.rsqrt(jnp.mean(v * v, axis=-1, keepdims=True) + 1e-06) * gains
        v = v.astype(BF16)
        for j in range(4):
            rows[b, 32 * j : 32 * j + 32, :] = v[:, 128 * j : 128 * j + 128]
    copies[2].wait()
    for b in range(0, lat.shape[0], 8):
        four = []
        for q in range(4):
            pair = [rot[b + q].astype(jnp.float32), rot[b + q + 4].astype(jnp.float32)]
            four.append(jnp.concatenate(pair, axis=-1))
        turned = jnp.concatenate(four, axis=0).astype(BF16).T
        for k in range(2):
            parts = [turned[64 * k + 16 * d : 64 * k + 16 * d + 16] for d in range(4)]
            for q, part in enumerate(regroup(parts)):
                rows[b + q + 4 * k, 128:144, :] = part
    copies[3].wait()
    copies[4].wait()


def ready(latents, rotary, gain, key_up, value_up):
    b = latents.shape[0]
    return call(
        ready_kernel,
        (shape(b, 144, 128), shape(1024, 128)),
        (latents, rotary, gain.reshape(1, -1), key_up.reshape(512, 128), value_up.reshape(512, 128)),
        in_specs=whole(5, pltpu.HBM),
        limit=67043328,
        scratch=[
            VMEM(latents.shape, BF16),
            VMEM(rotary.shape, BF16),
            VMEM((1, 512), jnp.float32),
            pltpu.SemaphoreType.DMA((5,)),
        ],
    )


def expand_kernel(along, *refs):
    rows, head, out, block, rotary = refs[:4], *refs[4:]
    s = block.shape[0]
    for i, hop in enumerate(HOPS):
        place = sender(along, hop)
        at = pl.multiple_of(place * 32, 32)
        for b in range(s):
            for j in range(4):
                block[b, pl.ds(at, 32), 128 * j : 128 * j + 128] = rows[i][b, 32 * j : 32 * j + 32]
            rotary[place, b] = rows[i][b, 128:144]
    w = jnp.concatenate([head[0:512, :], head[512:1024, :]], axis=-1)
    for b in range(0, s, 2):
        wide = jnp.dot(
            block[b : b + 2].reshape(256, 512), w, preferred_element_type=jnp.float32
        ).astype(BF16)
        for k in range(2):
            part = wide[128 * k : 128 * k + 128]
            out[b + k, 0:128] = part[:, 0:128].T
            for d, turned in enumerate(regroup([rotary[p, b + k] for p in range(SIDE)])):
                out[b + k, 128 + 16 * d : 144 + 16 * d] = turned
            out[b + k, 192:320] = part[:, 128:256]


def expand(rows, head, along):
    s = rows[0].shape[0]
    return call(
        functools.partial(expand_kernel, along),
        shape(s, 320, 128),
        (*rows, head),
        limit=8 * MIB,
        scratch=[VMEM((s, 128, 512), BF16), VMEM((SIDE, s, 16, 128), BF16)],
        flops=s * 128 * 512 * 256 * 2,
    )


def join_kernel(*refs):
    x_got, y_got, keys, values, sorted_, lined, sems = refs[:4], refs[4:8], *refs[8:]
    s = sorted_.shape[1]
    copies = []

    def copy(src, dst):
        copies.append(pltpu.make_async_copy(src, dst, sems.at[len(copies)]))
        copies[-1].start()

    for i, hop in enumerate(HOPS):
        y = sender("y", hop)
        copy(x_got[i].at[:, 192:320], values.at[0:s, y])
        for b in range(s):
            lanes = pl.ds(pl.multiple_of(b * 512 + y * 128, 128), 128)
            copy(x_got[i].at[b, 0:192], keys.at[:, lanes])
    for i, hop in enumerate(HOPS):
        x = sender("x", hop)
        rows = pl.ds(pl.multiple_of(x * 32, 32), 32)
        for y in range(SIDE):
            copy(y_got[i].at[:, 192 + 32 * y : 224 + 32 * y], values.at[s : 2 * s, y, rows])
        for b in range(s):
            sorted_[x, b] = y_got[i][b, 0:192]
    for b in range(s):
        for y, part in enumerate(regroup([sorted_[x, b] for x in range(SIDE)])):
            lined[b, :, 128 * y : 128 * y + 128] = part
        copy(lined.at[b], keys.at[:, (s + b) * 512 : (s + b + 1) * 512])
    for each in copies:
        each.wait()


def join(x_got, y_got):
    s = x_got[0].shape[0]
    return call(
        join_kernel,
        (shape(192, 2 * s * 512), shape(2 * s, SIDE, 128, 128)),
        (*x_got, *y_got),
        out_space=pltpu.HBM,
        limit=10 * MIB,
        scratch=[
            VMEM((SIDE, s, 192, 128), BF16),
            VMEM((s, 192, 512), BF16),
            pltpu.SemaphoreType.DMA((SIDE * (s + 1) + SIDE * SIDE + s,)),
        ],
        nbytes=8 * MIB,
    )


def named_move(array, along, i, back=False):
    return move(array, along, -HOPS[i] if back else HOPS[i])


def shards(latents, rotary_rows, latent_gain, key_up, value_up):
    rows, head = ready(latents, rotary_rows, latent_gain, key_up, value_up)
    mine = lax.all_to_all(rows, "seq", split_axis=0, concat_axis=0, tiled=True)
    heads = {a: [head] + [named_move(head, a, i, back=True) for i in (1, 2, 3)] for a in "xy"}
    mine, heads["x"][1] = lax.optimization_barrier((mine, heads["x"][1]))
    half = mine.shape[0] // 2
    near = {"x": [mine[:half]], "y": [mine[half:]]}
    for i in (1, 2, 3):
        for a in "xy":
            near[a].append(named_move(near[a][0], a, i))
    got = {"x": [None] * 4, "y": [None] * 4}
    for i in (3, 1, 2, 0):
        for a in "xy":
            piece = expand(near[a], heads[OTHER[a]][i], a)
            got[a][i] = named_move(piece, OTHER[a], i) if i else piece
    keys, values = join(got["x"], got["y"])
    return keys[None, None], values.reshape(1, -1, 1, 128)


def solution(mesh):
    return jax.shard_map(
        shards,
        mesh=mesh,
        in_specs=(
            P(None, ("seq", "tp"), None),
            P(None, ("seq", "tp"), None),
            P(),
            P(None, "tp", None),
            P(None, "tp", None),
        ),
        out_specs=(P("seq", "tp", None, None), P("seq", None, "tp", None)),
        check_vma=False,
    )
```

```python
import functools

import jax
import jax.numpy as jnp
from jax import lax
from jax.experimental import pallas as pl
from jax.experimental.pallas import tpu as pltpu
from jax.sharding import PartitionSpec as P


SIDE = 4
HOPS = (0, 1, -1, 2)
VMEM = pltpu.VMEM
MIB = 1 << 20
BF16 = jnp.bfloat16
OTHER = {"x": "y", "y": "x"}


def move(array, along, hop):
    pairs = []
    for y in range(SIDE):
        for x in range(SIDE):
            to = (y, (x + hop) % SIDE) if along == "x" else ((y + hop) % SIDE, x)
            pairs.append((y * SIDE + x, to[0] * SIDE + to[1]))
    return lax.ppermute(array, "tp", pairs)


def sender(along, hop):
    t = lax.axis_index("tp")
    mine = t % SIDE if along == "x" else t // SIDE
    return (mine - hop + SIDE) % SIDE


def whole(n, space=VMEM):
    return [pl.BlockSpec(memory_space=space)] * n


def shape(*dims):
    return jax.ShapeDtypeStruct(dims, BF16)


def call(kernel, outs, args, out_space=VMEM, in_specs=None, limit=24 * MIB, scratch=(), alias=None, flops=0, nbytes=MIB):
    return pl.pallas_call(
        kernel,
        out_shape=outs,
        in_specs=in_specs or whole(len(args)),
        out_specs=jax.tree.map(lambda _: pl.BlockSpec(memory_space=out_space), outs),
        scratch_shapes=list(scratch),
        input_output_aliases=alias or {},
        compiler_params=pltpu.CompilerParams(vmem_limit_bytes=limit),
        cost_estimate=pl.CostEstimate(flops=flops, bytes_accessed=nbytes, transcendentals=0),
    )(*args)


def regroup(parts):
    return [jnp.concatenate([p[:, 32 * k : 32 * k + 32] for p in parts], axis=-1) for k in range(4)]


def ready_kernel(lat_in, rot_in, gain_in, key_in, value_in, rows, weights, lat, rot, gain, sems):
    copies = [
        pltpu.make_async_copy(src, dst, sems.at[i])
        for i, (src, dst) in enumerate(
            (
                (lat_in, lat),
                (gain_in, gain),
                (rot_in, rot),
                (key_in, weights.at[0:512, :]),
                (value_in, weights.at[512:1024, :]),
            )
        )
    ]
    for copy in copies:
        copy.start()
    copies[0].wait()
    copies[1].wait()
    gains = gain[...]
    for b in range(lat.shape[0]):
        v = lat[b].astype(jnp.float32)
        v = v * lax.rsqrt(jnp.mean(v * v, axis=-1, keepdims=True) + 1e-06) * gains
        v = v.astype(BF16)
        for j in range(4):
            rows[b, 32 * j : 32 * j + 32, :] = v[:, 128 * j : 128 * j + 128]
    copies[2].wait()
    for b in range(0, lat.shape[0], 8):
        four = []
        for q in range(4):
            pair = [rot[b + q].astype(jnp.float32), rot[b + q + 4].astype(jnp.float32)]
            four.append(jnp.concatenate(pair, axis=-1))
        turned = jnp.concatenate(four, axis=0).astype(BF16).T
        for k in range(2):
            parts = [turned[64 * k + 16 * d : 64 * k + 16 * d + 16] for d in range(4)]
            for q, part in enumerate(regroup(parts)):
                rows[b + q + 4 * k, 128:144, :] = part
    copies[3].wait()
    copies[4].wait()


def ready(latents, rotary, gain, key_up, value_up):
    b = latents.shape[0]
    return call(
        ready_kernel,
        (shape(b, 144, 128), shape(1024, 128)),
        (latents, rotary, gain.reshape(1, -1), key_up.reshape(512, 128), value_up.reshape(512, 128)),
        in_specs=whole(5, pltpu.HBM),
        limit=67043328,
        scratch=[
            VMEM(latents.shape, BF16),
            VMEM(rotary.shape, BF16),
            VMEM((1, 512), jnp.float32),
            pltpu.SemaphoreType.DMA((5,)),
        ],
    )


def expand_kernel(n, *refs):
    rows, head, out = refs[:n], refs[n], refs[n + 1]
    w = jnp.concatenate([head[0:512, :], head[512:1024, :]], axis=-1)
    for i in range(n):
        a = rows[i]
        for g in range(a.shape[0] // 4):
            four = a[4 * g : 4 * g + 4]
            lhs = jnp.concatenate(
                [four[:, 32 * j : 32 * j + 32].reshape(128, 128) for j in range(4)], axis=-1
            )
            wide = jnp.dot(lhs, w, preferred_element_type=jnp.float32).astype(BF16)
            out[i, g, 0:128] = wide[:, 0:128].T
            for d, turned in enumerate(regroup([four[k, 128:144] for k in range(4)])):
                out[i, g, 128 + 16 * d : 144 + 16 * d] = turned
            out[i, g, 192:320] = wide[:, 128:256]


def expand(rows, head):
    n, s = len(rows), rows[0].shape[0]
    return call(
        functools.partial(expand_kernel, n),
        shape(n, s // 4, 320, 128),
        (*rows, head),
        limit=4 * MIB,
        flops=n * s * 32 * 512 * 256 * 2,
    )


def join_kernel(counts, *refs):
    pieces, (keys, values, sorted_, lined, sems) = refs[: sum(counts)], refs[sum(counts) :]
    groups = sorted_.shape[2]
    copies = []

    def copy(src, dst):
        copies.append(pltpu.make_async_copy(src, dst, sems.at[len(copies)]))
        copies[-1].start()

    at = 0
    for h, (outer, inner) in enumerate(("yx", "xy")):
        sources = []
        for o in range(len(HOPS)):
            mine = pieces[at : at + counts[h * 4 + o]]
            at += len(mine)
            sources.append([p.at[k] for p in mine for k in range(p.shape[0])])
        for o in range(4):
            for n in range(4):
                place = {outer: sender(outer, HOPS[o]), inner: sender(inner, HOPS[n])}
                rows = pl.ds(pl.multiple_of(place["x"] * 32, 32), 32)
                for g in range(groups):
                    for k in range(4):
                        copy(
                            sources[o][n].at[g, 192 + 32 * k : 224 + 32 * k],
                            values.at[(h * groups + g) * 4 + k, place["y"], rows],
                        )
        for o in range(4):
            for n in range(4):
                place = {outer: sender(outer, HOPS[o]), inner: sender(inner, HOPS[n])}
                slot = place["y"] * SIDE + place["x"]
                for g in range(groups):
                    sorted_[h, slot, g] = sources[o][n][g, 0:192]
        for g in range(groups):
            for y in range(SIDE):
                parts = [sorted_[h, y * SIDE + x, g] for x in range(SIDE)]
                for k, part in enumerate(regroup(parts)):
                    lined[h * groups + g, :, 512 * k + 128 * y : 512 * k + 128 * y + 128] = part
            first = (h * groups + g) * 2048
            copy(lined.at[h * groups + g], keys.at[:, first : first + 2048])
    for each in copies:
        each.wait()


def join(x_got, y_got):
    groups = x_got[0][0].shape[1]
    got = x_got + y_got
    return call(
        functools.partial(join_kernel, tuple(map(len, got))),
        (shape(192, 2 * groups * 2048), shape(2 * groups * 4, SIDE, 128, 128)),
        sum(got, []),
        out_space=pltpu.HBM,
        limit=16 * MIB,
        scratch=[
            VMEM((2, SIDE * SIDE, groups, 192, 128), BF16),
            VMEM((2 * groups, 192, 2048), BF16),
            pltpu.SemaphoreType.DMA((2 * groups * (SIDE * SIDE * 4 + 1),)),
        ],
        nbytes=8 * MIB,
    )


def named_move(array, along, i, back=False):
    return move(array, along, -HOPS[i] if back else HOPS[i])


def shards(latents, rotary_rows, latent_gain, key_up, value_up):
    rows, head = ready(latents, rotary_rows, latent_gain, key_up, value_up)
    mine = lax.all_to_all(rows, "seq", split_axis=0, concat_axis=0, tiled=True)
    heads = {a: [head] + [named_move(head, a, i, back=True) for i in (1, 2, 3)] for a in "xy"}
    mine, heads["x"][1] = lax.optimization_barrier((mine, heads["x"][1]))
    half = mine.shape[0] // 2
    near = {"x": [mine[:half]], "y": [mine[half:]]}
    for i in (1, 2, 3):
        for a in "xy":
            near[a].append(named_move(near[a][0], a, i))
    got = {"x": [None] * 4, "y": [None] * 4}
    ahead = {}
    for a in "yx":
        ahead[a] = expand(near[a][:1], heads[OTHER[a]][3])
    for a in "yx":
        ahead[a] = named_move(ahead[a], OTHER[a], 3)
    for i in (3, 1, 2, 0):
        for a in "xy":
            piece = expand(near[a][1:] if i == 3 else near[a], heads[OTHER[a]][i])
            got[a][i] = [named_move(piece, OTHER[a], i) if i else piece]
    for a in "xy":
        got[a][3].insert(0, ahead[a])
    keys, values = join(got["x"], got["y"])
    return keys[None, None], values.reshape(1, -1, 1, 128)


def solution(mesh):
    return jax.shard_map(
        shards,
        mesh=mesh,
        in_specs=(
            P(None, ("seq", "tp"), None),
            P(None, ("seq", "tp"), None),
            P(),
            P(None, "tp", None),
            P(None, "tp", None),
        ),
        out_specs=(P("seq", "tp", None, None), P("seq", None, "tp", None)),
        check_vma=False,
    )
```

```python
import functools

import jax
import jax.numpy as jnp
from jax import lax
from jax.experimental import pallas as pl
from jax.experimental.pallas import tpu as pltpu
from jax.sharding import PartitionSpec as P


SIDE = 4
HOPS = (0, 1, -1, 2)
VMEM = pltpu.VMEM
MIB = 1 << 20
BF16 = jnp.bfloat16
OTHER = {"x": "y", "y": "x"}


def move(array, along, hop):
    pairs = []
    for y in range(SIDE):
        for x in range(SIDE):
            to = (y, (x + hop) % SIDE) if along == "x" else ((y + hop) % SIDE, x)
            pairs.append((y * SIDE + x, to[0] * SIDE + to[1]))
    return lax.ppermute(array, "tp", pairs)


def sender(along, hop):
    t = lax.axis_index("tp")
    mine = t % SIDE if along == "x" else t // SIDE
    return (mine - hop + SIDE) % SIDE


def whole(n, space=VMEM):
    return [pl.BlockSpec(memory_space=space)] * n


def shape(*dims):
    return jax.ShapeDtypeStruct(dims, BF16)


def call(kernel, outs, args, out_space=VMEM, in_specs=None, limit=24 * MIB, scratch=(), alias=None, flops=0, nbytes=MIB):
    return pl.pallas_call(
        kernel,
        out_shape=outs,
        in_specs=in_specs or whole(len(args)),
        out_specs=jax.tree.map(lambda _: pl.BlockSpec(memory_space=out_space), outs),
        scratch_shapes=list(scratch),
        input_output_aliases=alias or {},
        compiler_params=pltpu.CompilerParams(vmem_limit_bytes=limit),
        cost_estimate=pl.CostEstimate(flops=flops, bytes_accessed=nbytes, transcendentals=0),
    )(*args)


def regroup(parts):
    return [jnp.concatenate([p[:, 32 * k : 32 * k + 32] for p in parts], axis=-1) for k in range(4)]


def ready_kernel(lat_in, rot_in, gain_in, key_in, value_in, rows, weights, lat, rot, gain, sems):
    copies = [
        pltpu.make_async_copy(src, dst, sems.at[i])
        for i, (src, dst) in enumerate(
            (
                (lat_in, lat),
                (gain_in, gain),
                (rot_in, rot),
                (key_in, weights.at[0:512, :]),
                (value_in, weights.at[512:1024, :]),
            )
        )
    ]
    for copy in copies:
        copy.start()
    copies[0].wait()
    copies[1].wait()
    gains = gain[...]
    for b in range(lat.shape[0]):
        v = lat[b].astype(jnp.float32)
        v = v * lax.rsqrt(jnp.mean(v * v, axis=-1, keepdims=True) + 1e-06) * gains
        v = v.astype(BF16)
        for j in range(4):
            rows[b, 32 * j : 32 * j + 32, :] = v[:, 128 * j : 128 * j + 128]
    copies[2].wait()
    for b in range(0, lat.shape[0], 8):
        four = []
        for q in range(4):
            pair = [rot[b + q].astype(jnp.float32), rot[b + q + 4].astype(jnp.float32)]
            four.append(jnp.concatenate(pair, axis=-1))
        turned = jnp.concatenate(four, axis=0).astype(BF16).T
        for k in range(2):
            parts = [turned[64 * k + 16 * d : 64 * k + 16 * d + 16] for d in range(4)]
            for q, part in enumerate(regroup(parts)):
                rows[b + q + 4 * k, 128:144, :] = part
    copies[3].wait()
    copies[4].wait()


def ready(latents, rotary, gain, key_up, value_up):
    b = latents.shape[0]
    return call(
        ready_kernel,
        (shape(b, 144, 128), shape(1024, 128)),
        (latents, rotary, gain.reshape(1, -1), key_up.reshape(512, 128), value_up.reshape(512, 128)),
        in_specs=whole(5, pltpu.HBM),
        limit=67043328,
        scratch=[
            VMEM(latents.shape, BF16),
            VMEM(rotary.shape, BF16),
            VMEM((1, 512), jnp.float32),
            pltpu.SemaphoreType.DMA((5,)),
        ],
    )


def expand_kernel(n, *refs):
    rows, head, out = refs[:n], refs[n], refs[n + 1]
    w = jnp.concatenate([head[0:512, :], head[512:1024, :]], axis=-1)
    for i in range(n):
        a = rows[i]
        for g in range(a.shape[0] // 4):
            four = a[4 * g : 4 * g + 4]
            lhs = jnp.concatenate(
                [four[:, 32 * j : 32 * j + 32].reshape(128, 128) for j in range(4)], axis=-1
            )
            wide = jnp.dot(lhs, w, preferred_element_type=jnp.float32).astype(BF16)
            out[i, g, 0:4] = wide[:, 0:128].T.reshape(4, 32, 128)
            turned = jnp.concatenate(regroup([four[k, 128:144] for k in range(4)]), axis=0)
            out[i, g, 4:6] = turned.reshape(2, 32, 128)
            out[i, g, 6:10] = wide[:, 128:256].reshape(4, 32, 128)


def expand(rows, head):
    n, s = len(rows), rows[0].shape[0]
    return call(
        functools.partial(expand_kernel, n),
        shape(n, s // 4, 10, 32, 128),
        (*rows, head),
        limit=4 * MIB,
        flops=n * s * 32 * 512 * 256 * 2,
    )


def join_kernel(counts, *refs):
    pieces, (keys, values, sorted_, lined, sems) = refs[: sum(counts)], refs[sum(counts) :]
    groups = sorted_.shape[2]
    copies = []

    def copy(src, dst):
        copies.append(pltpu.make_async_copy(src, dst, sems.at[len(copies)]))
        copies[-1].start()

    at = 0
    for h, (outer, inner) in enumerate(("yx", "xy")):
        sources = []
        for o in range(len(HOPS)):
            mine = pieces[at : at + counts[h * 4 + o]]
            at += len(mine)
            sources.append([p.at[k] for p in mine for k in range(p.shape[0])])
        for o in range(4):
            for n in range(4):
                place = {outer: sender(outer, HOPS[o]), inner: sender(inner, HOPS[n])}
                rows = pl.ds(pl.multiple_of(place["x"] * 32, 32), 32)
                for g in range(groups):
                    to = (h * groups + g) * 4
                    copy(sources[o][n].at[g, 6:10], values.at[to : to + 4, place["y"], rows])
        for o in range(4):
            for n in range(4):
                place = {outer: sender(outer, HOPS[o]), inner: sender(inner, HOPS[n])}
                slot = place["y"] * SIDE + place["x"]
                for g in range(groups):
                    sorted_[h, slot, g] = sources[o][n][g, 0:6].reshape(192, 128)
        for g in range(groups):
            for y in range(SIDE):
                parts = [sorted_[h, y * SIDE + x, g] for x in range(SIDE)]
                for k, part in enumerate(regroup(parts)):
                    lined[h * groups + g, :, 512 * k + 128 * y : 512 * k + 128 * y + 128] = part
            first = (h * groups + g) * 2048
            copy(lined.at[h * groups + g], keys.at[:, first : first + 2048])
    for each in copies:
        each.wait()


def join(x_got, y_got):
    groups = x_got[0][0].shape[1]
    got = x_got + y_got
    return call(
        functools.partial(join_kernel, tuple(map(len, got))),
        (shape(192, 2 * groups * 2048), shape(2 * groups * 4, SIDE, 128, 128)),
        sum(got, []),
        out_space=pltpu.HBM,
        limit=16 * MIB,
        scratch=[
            VMEM((2, SIDE * SIDE, groups, 192, 128), BF16),
            VMEM((2 * groups, 192, 2048), BF16),
            pltpu.SemaphoreType.DMA((2 * groups * (SIDE * SIDE + 1),)),
        ],
        nbytes=8 * MIB,
    )


def named_move(array, along, i, back=False):
    return move(array, along, -HOPS[i] if back else HOPS[i])


def shards(latents, rotary_rows, latent_gain, key_up, value_up):
    rows, head = ready(latents, rotary_rows, latent_gain, key_up, value_up)
    mine = lax.all_to_all(rows, "seq", split_axis=0, concat_axis=0, tiled=True)
    heads = {a: [head] + [named_move(head, a, i, back=True) for i in (1, 2, 3)] for a in "xy"}
    mine, heads["x"][1] = lax.optimization_barrier((mine, heads["x"][1]))
    half = mine.shape[0] // 2
    near = {"x": [mine[:half]], "y": [mine[half:]]}
    for i in (1, 2, 3):
        for a in "xy":
            near[a].append(named_move(near[a][0], a, i))
    got = {"x": [None] * 4, "y": [None] * 4}
    ahead = {"x": [None] * 4, "y": [None] * 4}
    for i in (3, 1, 2):
        for a in "yx":
            ahead[a][i] = expand(near[a][:1], heads[OTHER[a]][i])
            ahead[a][i] = named_move(ahead[a][i], OTHER[a], i)
    for i in (3, 1, 2, 0):
        for a in "yx":
            piece = expand(near[a][1:] if i else near[a], heads[OTHER[a]][i])
            got[a][i] = [ahead[a][i], named_move(piece, OTHER[a], i)] if i else [piece]
    keys, values = join(got["x"], got["y"])
    return keys[None, None], values.reshape(1, -1, 1, 128)


def solution(mesh):
    return jax.shard_map(
        shards,
        mesh=mesh,
        in_specs=(
            P(None, ("seq", "tp"), None),
            P(None, ("seq", "tp"), None),
            P(),
            P(None, "tp", None),
            P(None, "tp", None),
        ),
        out_specs=(P("seq", "tp", None, None), P("seq", None, "tp", None)),
        check_vma=False,
    )
```

```python
import functools

import jax
import jax.numpy as jnp
from jax import lax
from jax.experimental import pallas as pl
from jax.experimental.pallas import tpu as pltpu
from jax.sharding import PartitionSpec as P


SIDE = 4
HOPS = (0, 1, -1, 2)
VMEM = pltpu.VMEM
MIB = 1 << 20
BF16 = jnp.bfloat16
OTHER = {"x": "y", "y": "x"}


def move(array, along, hop):
    pairs = []
    for y in range(SIDE):
        for x in range(SIDE):
            to = (y, (x + hop) % SIDE) if along == "x" else ((y + hop) % SIDE, x)
            pairs.append((y * SIDE + x, to[0] * SIDE + to[1]))
    return lax.ppermute(array, "tp", pairs)


def sender(along, hop):
    t = lax.axis_index("tp")
    mine = t % SIDE if along == "x" else t // SIDE
    return (mine - hop + SIDE) % SIDE


def whole(n, space=VMEM):
    return [pl.BlockSpec(memory_space=space)] * n


def shape(*dims):
    return jax.ShapeDtypeStruct(dims, BF16)


def call(kernel, outs, args, out_space=VMEM, in_specs=None, limit=24 * MIB, scratch=(), alias=None, flops=0, nbytes=MIB):
    return pl.pallas_call(
        kernel,
        out_shape=outs,
        in_specs=in_specs or whole(len(args)),
        out_specs=jax.tree.map(lambda _: pl.BlockSpec(memory_space=out_space), outs),
        scratch_shapes=list(scratch),
        input_output_aliases=alias or {},
        compiler_params=pltpu.CompilerParams(vmem_limit_bytes=limit),
        cost_estimate=pl.CostEstimate(flops=flops, bytes_accessed=nbytes, transcendentals=0),
    )(*args)


def regroup(parts):
    return [jnp.concatenate([p[:, 32 * k : 32 * k + 32] for p in parts], axis=-1) for k in range(4)]


def ready_kernel(lat_in, rot_in, gain_in, key_in, value_in, rows, weights, lat, rot, gain, sems):
    copies = [
        pltpu.make_async_copy(src, dst, sems.at[i])
        for i, (src, dst) in enumerate(
            (
                (lat_in, lat),
                (gain_in, gain),
                (rot_in, rot),
                (key_in, weights.at[0:512, :]),
                (value_in, weights.at[512:1024, :]),
            )
        )
    ]
    for copy in copies:
        copy.start()
    copies[0].wait()
    copies[1].wait()
    gains = gain[...]
    for b in range(lat.shape[0]):
        v = lat[b].astype(jnp.float32)
        v = v * lax.rsqrt(jnp.mean(v * v, axis=-1, keepdims=True) + 1e-06) * gains
        v = v.astype(BF16)
        for j in range(4):
            rows[b, 32 * j : 32 * j + 32, :] = v[:, 128 * j : 128 * j + 128]
    copies[2].wait()
    for b in range(0, lat.shape[0], 8):
        four = []
        for q in range(4):
            pair = [rot[b + q].astype(jnp.float32), rot[b + q + 4].astype(jnp.float32)]
            four.append(jnp.concatenate(pair, axis=-1))
        turned = jnp.concatenate(four, axis=0).astype(BF16).T
        for k in range(2):
            parts = [turned[64 * k + 16 * d : 64 * k + 16 * d + 16] for d in range(4)]
            for q, part in enumerate(regroup(parts)):
                rows[b + q + 4 * k, 128:144, :] = part
    copies[3].wait()
    copies[4].wait()


def ready(latents, rotary, gain, key_up, value_up):
    b = latents.shape[0]
    return call(
        ready_kernel,
        (shape(b, 144, 128), shape(1024, 128)),
        (latents, rotary, gain.reshape(1, -1), key_up.reshape(512, 128), value_up.reshape(512, 128)),
        in_specs=whole(5, pltpu.HBM),
        limit=67043328,
        scratch=[
            VMEM(latents.shape, BF16),
            VMEM(rotary.shape, BF16),
            VMEM((1, 512), jnp.float32),
            pltpu.SemaphoreType.DMA((5,)),
        ],
    )


def expand_kernel(n, *refs):
    rows, head, out = refs[:n], refs[n], refs[n + 1]
    w = jnp.concatenate([head[0:512, :], head[512:1024, :]], axis=-1)
    for i in range(n):
        a = rows[i]
        for g in range(a.shape[0] // 4):
            four = a[4 * g : 4 * g + 4]
            lhs = jnp.concatenate(
                [four[:, 32 * j : 32 * j + 32].reshape(128, 128) for j in range(4)], axis=-1
            )
            wide = jnp.dot(lhs, w, preferred_element_type=jnp.float32).astype(BF16)
            out[i, g, 0:4] = wide[:, 0:128].T.reshape(4, 32, 128)
            turned = jnp.concatenate(regroup([four[k, 128:144] for k in range(4)]), axis=0)
            out[i, g, 4:6] = turned.reshape(2, 32, 128)
            out[i, g, 6:10] = wide[:, 128:256].reshape(4, 32, 128)


def expand(rows, head):
    n, s = len(rows), rows[0].shape[0]
    return call(
        functools.partial(expand_kernel, n),
        shape(n, s // 4, 10, 32, 128),
        (*rows, head),
        limit=4 * MIB,
        flops=n * s * 32 * 512 * 256 * 2,
    )


def join_kernel(first, outer, inner, counts, *refs):
    pieces, (keys, values, sorted_, lined, sems) = refs[: sum(counts)], refs[-5:]
    groups = sorted_.shape[1]
    copies = []

    def copy(src, dst):
        copies.append(pltpu.make_async_copy(src, dst, sems.at[len(copies)]))
        copies[-1].start()

    at = 0
    for o in range(len(HOPS)):
        mine = pieces[at : at + counts[o]]
        at += len(mine)
        units = [p.at[k] for p in mine for k in range(p.shape[0])]
        for n, unit in enumerate(units):
            place = {outer: sender(outer, HOPS[o]), inner: sender(inner, HOPS[n])}
            rows = pl.ds(pl.multiple_of(place["x"] * 32, 32), 32)
            slot = place["y"] * SIDE + place["x"]
            for g in range(groups):
                to = first + 4 * g
                copy(unit.at[g, 6:10], values.at[to : to + 4, place["y"], rows])
                sorted_[slot, g] = unit[g, 0:6].reshape(192, 128)
    for g in range(groups):
        for y in range(SIDE):
            parts = [sorted_[y * SIDE + x, g] for x in range(SIDE)]
            for k, part in enumerate(regroup(parts)):
                lined[g, :, 512 * k + 128 * y : 512 * k + 128 * y + 128] = part
        at = (first + 4 * g) * 512
        copy(lined.at[g], keys.at[:, at : at + 2048])
    for each in copies:
        each.wait()


def join(got, first, outer, inner, before=()):
    pieces = sum(got, [])
    groups = got[0][0].shape[1]
    n = len(pieces)
    return call(
        functools.partial(join_kernel, first, outer, inner, tuple(map(len, got))),
        (shape(192, 2 * groups * 2048), shape(2 * groups * 4, SIDE, 128, 128)),
        (*pieces, *before),
        in_specs=whole(n) + whole(len(before), pltpu.HBM),
        out_space=pltpu.HBM,
        limit=8 * MIB,
        scratch=[
            VMEM((SIDE * SIDE, groups, 192, 128), BF16),
            VMEM((groups, 192, 2048), BF16),
            pltpu.SemaphoreType.DMA((groups * (SIDE * SIDE + 1),)),
        ],
        alias={n + k: k for k in range(len(before))},
        nbytes=4 * MIB,
    )


def named_move(array, along, i, back=False):
    return move(array, along, -HOPS[i] if back else HOPS[i])


def shards(latents, rotary_rows, latent_gain, key_up, value_up):
    rows, head = ready(latents, rotary_rows, latent_gain, key_up, value_up)
    mine = lax.all_to_all(rows, "seq", split_axis=0, concat_axis=0, tiled=True)
    heads = {a: [head] + [named_move(head, a, i, back=True) for i in (1, 2, 3)] for a in "xy"}
    mine, heads["x"][1] = lax.optimization_barrier((mine, heads["x"][1]))
    half = mine.shape[0] // 2
    near = {"x": [mine[:half]], "y": [mine[half:]]}
    for i in (1, 2, 3):
        for a in "xy":
            near[a].append(named_move(near[a][0], a, i))
    got = {"x": [None] * 4, "y": [None] * 4}
    ahead = {"x": [None] * 4, "y": [None] * 4}
    for i in (3, 1, 2):
        for a in "yx":
            ahead[a][i] = expand(near[a][:1], heads[OTHER[a]][i])
            ahead[a][i] = named_move(ahead[a][i], OTHER[a], i)
    for i in (3, 1, 2, 0):
        for a in "yx":
            piece = expand(near[a][1:] if i else near[a], heads[OTHER[a]][i])
            got[a][i] = [ahead[a][i], named_move(piece, OTHER[a], i)] if i else [piece]
    outs = join(got["y"], half, "x", "y")
    keys, values = join(got["x"], 0, "y", "x", outs)
    return keys[None, None], values.reshape(1, -1, 1, 128)


def solution(mesh):
    return jax.shard_map(
        shards,
        mesh=mesh,
        in_specs=(
            P(None, ("seq", "tp"), None),
            P(None, ("seq", "tp"), None),
            P(),
            P(None, "tp", None),
            P(None, "tp", None),
        ),
        out_specs=(P("seq", "tp", None, None), P("seq", None, "tp", None)),
        check_vma=False,
    )
```

```python
import functools

import jax
import jax.numpy as jnp
from jax import lax
from jax.experimental import pallas as pl
from jax.experimental.pallas import tpu as pltpu
from jax.sharding import PartitionSpec as P


SIDE = 4
HOPS = (0, 1, -1, 2)
VMEM = pltpu.VMEM
MIB = 1 << 20
BF16 = jnp.bfloat16
OTHER = {"x": "y", "y": "x"}


def move(array, along, hop):
    pairs = []
    for y in range(SIDE):
        for x in range(SIDE):
            to = (y, (x + hop) % SIDE) if along == "x" else ((y + hop) % SIDE, x)
            pairs.append((y * SIDE + x, to[0] * SIDE + to[1]))
    return lax.ppermute(array, "tp", pairs)


def sender(along, hop):
    t = lax.axis_index("tp")
    mine = t % SIDE if along == "x" else t // SIDE
    return (mine - hop + SIDE) % SIDE


def whole(n, space=VMEM):
    return [pl.BlockSpec(memory_space=space)] * n


def shape(*dims):
    return jax.ShapeDtypeStruct(dims, BF16)


def call(kernel, outs, args, out_space=VMEM, in_specs=None, limit=24 * MIB, scratch=(), alias=None, flops=0, nbytes=MIB):
    return pl.pallas_call(
        kernel,
        out_shape=outs,
        in_specs=in_specs or whole(len(args)),
        out_specs=jax.tree.map(lambda _: pl.BlockSpec(memory_space=out_space), outs),
        scratch_shapes=list(scratch),
        input_output_aliases=alias or {},
        compiler_params=pltpu.CompilerParams(vmem_limit_bytes=limit),
        cost_estimate=pl.CostEstimate(flops=flops, bytes_accessed=nbytes, transcendentals=0),
    )(*args)


def regroup(parts):
    return [jnp.concatenate([p[:, 32 * k : 32 * k + 32] for p in parts], axis=-1) for k in range(4)]


def ready_kernel(lat_in, rot_in, gain_in, key_in, value_in, rows, weights, lat, rot, gain, sems):
    copies = [
        pltpu.make_async_copy(src, dst, sems.at[i])
        for i, (src, dst) in enumerate(
            (
                (lat_in, lat),
                (gain_in, gain),
                (rot_in, rot),
                (key_in, weights.at[0:512, :]),
                (value_in, weights.at[512:1024, :]),
            )
        )
    ]
    for copy in copies:
        copy.start()
    copies[0].wait()
    copies[1].wait()
    gains = gain[...]
    for b in range(lat.shape[0]):
        v = lat[b].astype(jnp.float32)
        v = v * lax.rsqrt(jnp.mean(v * v, axis=-1, keepdims=True) + 1e-06) * gains
        v = v.astype(BF16)
        for j in range(4):
            rows[b, 32 * j : 32 * j + 32, :] = v[:, 128 * j : 128 * j + 128]
    copies[2].wait()
    for b in range(0, lat.shape[0], 8):
        four = []
        for q in range(4):
            pair = [rot[b + q].astype(jnp.float32), rot[b + q + 4].astype(jnp.float32)]
            four.append(jnp.concatenate(pair, axis=-1))
        turned = jnp.concatenate(four, axis=0).astype(BF16).T
        for k in range(2):
            parts = [turned[64 * k + 16 * d : 64 * k + 16 * d + 16] for d in range(4)]
            for q, part in enumerate(regroup(parts)):
                rows[b + q + 4 * k, 128:144, :] = part
    copies[3].wait()
    copies[4].wait()


def ready(latents, rotary, gain, key_up, value_up):
    b = latents.shape[0]
    return call(
        ready_kernel,
        (shape(b, 144, 128), shape(1024, 128)),
        (latents, rotary, gain.reshape(1, -1), key_up.reshape(512, 128), value_up.reshape(512, 128)),
        in_specs=whole(5, pltpu.HBM),
        limit=67043328,
        scratch=[
            VMEM(latents.shape, BF16),
            VMEM(rotary.shape, BF16),
            VMEM((1, 512), jnp.float32),
            pltpu.SemaphoreType.DMA((5,)),
        ],
    )


def expand_kernel(n, *refs):
    rows, head, out = refs[:n], refs[n], refs[n + 1]
    w = jnp.concatenate([head[0:512, :], head[512:1024, :]], axis=-1)
    for i in range(n):
        a = rows[i]
        for g in range(a.shape[0] // 4):
            four = a[4 * g : 4 * g + 4]
            lhs = jnp.concatenate(
                [four[:, 32 * j : 32 * j + 32].reshape(128, 128) for j in range(4)], axis=-1
            )
            wide = jnp.dot(lhs, w, preferred_element_type=jnp.float32).astype(BF16)
            out[i, g, 0:4] = wide[:, 0:128].T.reshape(4, 32, 128)
            turned = jnp.concatenate(regroup([four[k, 128:144] for k in range(4)]), axis=0)
            out[i, g, 4:6] = turned.reshape(2, 32, 128)
            out[i, g, 6:10] = wide[:, 128:256].reshape(4, 32, 128)


def expand(rows, head):
    n, s = len(rows), rows[0].shape[0]
    return call(
        functools.partial(expand_kernel, n),
        shape(n, s // 4, 10, 32, 128),
        (*rows, head),
        limit=4 * MIB,
        flops=n * s * 32 * 512 * 256 * 2,
    )


def copier(copies, sems):
    def copy(src, dst):
        copies.append(pltpu.make_async_copy(src, dst, sems.at[len(copies)]))
        copies[-1].start()

    return copy


def spot(outer, inner, o, n):
    place = {outer: sender(outer, HOPS[o]), inner: sender(inner, HOPS[n])}
    return place["y"], place["x"]


def put_values(copy, values, unit, first, y, x):
    for g in range(unit.shape[0]):
        to = first + 4 * g
        rows = pl.ds(pl.multiple_of(x * 32, 32), 32)
        copy(unit.at[g, 6:10], values.at[to : to + 4, y, rows])


def line_keys(lined, sorted_, g):
    for y in range(SIDE):
        parts = [sorted_[y * SIDE + x, g] for x in range(SIDE)]
        for k, part in enumerate(regroup(parts)):
            lined[g, k, :, 128 * y : 128 * y + 128] = part


def sort_keys(sorted_, pieces, outer, inner):
    for o in range(len(HOPS)):
        mine = [pieces.pop(0) for _ in range(2 if o else 1)]
        units = [p.at[k] for p in mine for k in range(p.shape[0])]
        for n, unit in enumerate(units):
            y, x = spot(outer, inner, o, n)
            for g in range(sorted_.shape[1]):
                sorted_[y * SIDE + x, g] = unit[g, 0:6].reshape(192, 128)


def early_kernel(*refs):
    pieces, values, sems = list(refs[:8]), refs[8], refs[9]
    copies = []
    copy = copier(copies, sems)
    for h, (outer, inner) in enumerate(("xy", "yx")):
        first = (1 - h) * values.shape[0] // 2
        for o in range(4):
            piece = pieces.pop(0)
            for n in range(piece.shape[0]):
                put_values(copy, values, piece.at[n], first, *spot(outer, inner, o, n))
    for each in copies:
        each.wait()


def line_kernel(*refs):
    pieces, lined, sorted_ = list(refs[:-2]), refs[-2], refs[-1]
    sort_keys(sorted_, pieces, "x", "y")
    for g in range(lined.shape[0]):
        line_keys(lined, sorted_, g)


def join_kernel(*refs):
    y_rest, x_pieces, y_lined = refs[:3], list(refs[3:10]), refs[10]
    keys, values, sorted_, lined, sems = refs[12:]
    groups = lined.shape[0]
    copies = []
    copy = copier(copies, sems)
    for g in range(groups):
        for k in range(4):
            at = (4 * (groups + g) + k) * 512
            copy(y_lined.at[g, k], keys.at[:, at : at + 512])
    for (outer, inner), first, rest in (("xy", 4 * groups, y_rest), ("yx", 0, x_pieces[2::2])):
        for o, piece in enumerate(rest):
            for n in range(piece.shape[0]):
                put_values(copy, values, piece.at[n], first, *spot(outer, inner, o + 1, n + 1))
    sort_keys(sorted_, x_pieces, "y", "x")
    for g in range(groups):
        line_keys(lined, sorted_, g)
        for k in range(4):
            at = (4 * g + k) * 512
            copy(lined.at[g, k], keys.at[:, at : at + 512])
    for each in copies:
        each.wait()


def finish(y_got, x_got):
    groups = y_got[0][0].shape[1]
    keys, values = shape(192, 2 * groups * 2048), shape(2 * groups * 4, SIDE, 128, 128)
    lined = (groups, 4, 192, 512)
    sorting = VMEM((SIDE * SIDE, groups, 192, 128), BF16)
    sems = pltpu.SemaphoreType.DMA
    started = call(
        early_kernel,
        values,
        [p[0] for p in y_got + x_got],
        out_space=pltpu.HBM,
        limit=MIB,
        scratch=[sems((2 * 7 * groups,))],
        nbytes=2 * MIB,
    )
    y_lined = call(
        line_kernel, shape(*lined), sum(y_got, []), limit=4 * MIB, scratch=[sorting], nbytes=3 * MIB
    )
    args = [p[1] for p in y_got[1:]] + sum(x_got, []) + [y_lined, started]
    return call(
        join_kernel,
        (keys, values),
        args,
        in_specs=whole(len(args) - 1) + whole(1, pltpu.HBM),
        out_space=pltpu.HBM,
        limit=6 * MIB,
        scratch=[sorting, VMEM(lined, BF16), sems((groups * (8 + 18),))],
        alias={len(args) - 1: 1},
        nbytes=6 * MIB,
    )


def named_move(array, along, i, back=False):
    return move(array, along, -HOPS[i] if back else HOPS[i])


def shards(latents, rotary_rows, latent_gain, key_up, value_up):
    rows, head = ready(latents, rotary_rows, latent_gain, key_up, value_up)
    mine = lax.all_to_all(rows, "seq", split_axis=0, concat_axis=0, tiled=True)
    heads = {a: [head] + [named_move(head, a, i, back=True) for i in (1, 2, 3)] for a in "xy"}
    mine, heads["x"][1] = lax.optimization_barrier((mine, heads["x"][1]))
    half = mine.shape[0] // 2
    near = {"x": [mine[:half]], "y": [mine[half:]]}
    for i in (1, 2, 3):
        for a in "xy":
            near[a].append(named_move(near[a][0], a, i))
    got = {"x": [None] * 4, "y": [None] * 4}
    ahead = {"x": [None] * 4, "y": [None] * 4}
    for i in (3, 1, 2):
        for a in "yx":
            ahead[a][i] = expand(near[a][:1], heads[OTHER[a]][i])
            ahead[a][i] = named_move(ahead[a][i], OTHER[a], i)
    for i in (3, 1, 2, 0):
        for a in "yx":
            piece = expand(near[a][1:] if i else near[a], heads[OTHER[a]][i])
            got[a][i] = [ahead[a][i], named_move(piece, OTHER[a], i)] if i else [piece]
    keys, values = finish(got["y"], got["x"])
    return keys[None, None], values.reshape(1, -1, 1, 128)


def solution(mesh):
    return jax.shard_map(
        shards,
        mesh=mesh,
        in_specs=(
            P(None, ("seq", "tp"), None),
            P(None, ("seq", "tp"), None),
            P(),
            P(None, "tp", None),
            P(None, "tp", None),
        ),
        out_specs=(P("seq", "tp", None, None), P("seq", None, "tp", None)),
        check_vma=False,
    )
```

```python
import functools

import jax
import jax.numpy as jnp
from jax import lax
from jax.experimental import pallas as pl
from jax.experimental.pallas import tpu as pltpu
from jax.sharding import PartitionSpec as P


SIDE = 4
HOPS = (0, 1, -1, 2)
VMEM = pltpu.VMEM
MIB = 1 << 20
BF16 = jnp.bfloat16
OTHER = {"x": "y", "y": "x"}


def move(array, along, hop):
    pairs = []
    for y in range(SIDE):
        for x in range(SIDE):
            to = (y, (x + hop) % SIDE) if along == "x" else ((y + hop) % SIDE, x)
            pairs.append((y * SIDE + x, to[0] * SIDE + to[1]))
    return lax.ppermute(array, "tp", pairs)


def sender(along, hop):
    t = lax.axis_index("tp")
    mine = t % SIDE if along == "x" else t // SIDE
    return (mine - hop + SIDE) % SIDE


def whole(n, space=VMEM):
    return [pl.BlockSpec(memory_space=space)] * n


def shape(*dims):
    return jax.ShapeDtypeStruct(dims, BF16)


def call(kernel, outs, args, out_space=VMEM, in_specs=None, limit=24 * MIB, scratch=(), alias=None, flops=0, nbytes=MIB):
    return pl.pallas_call(
        kernel,
        out_shape=outs,
        in_specs=in_specs or whole(len(args)),
        out_specs=jax.tree.map(lambda _: pl.BlockSpec(memory_space=out_space), outs),
        scratch_shapes=list(scratch),
        input_output_aliases=alias or {},
        compiler_params=pltpu.CompilerParams(vmem_limit_bytes=limit),
        cost_estimate=pl.CostEstimate(flops=flops, bytes_accessed=nbytes, transcendentals=0),
    )(*args)


def regroup(parts):
    return [jnp.concatenate([p[:, 32 * k : 32 * k + 32] for p in parts], axis=-1) for k in range(4)]


def ready_kernel(lat_in, rot_in, gain_in, key_in, value_in, rows, weights, lat, rot, gain, sems):
    copies = [
        pltpu.make_async_copy(src, dst, sems.at[i])
        for i, (src, dst) in enumerate(
            (
                (lat_in, lat),
                (gain_in, gain),
                (rot_in, rot),
                (key_in, weights.at[0:512, :]),
                (value_in, weights.at[512:1024, :]),
            )
        )
    ]
    for copy in copies:
        copy.start()
    copies[0].wait()
    copies[1].wait()
    gains = gain[...]
    for b in range(lat.shape[0]):
        v = lat[b].astype(jnp.float32)
        v = v * lax.rsqrt(jnp.mean(v * v, axis=-1, keepdims=True) + 1e-06) * gains
        v = v.astype(BF16)
        for j in range(4):
            rows[b, 32 * j : 32 * j + 32, :] = v[:, 128 * j : 128 * j + 128]
    copies[2].wait()
    for b in range(0, lat.shape[0], 8):
        four = []
        for q in range(4):
            pair = [rot[b + q].astype(jnp.float32), rot[b + q + 4].astype(jnp.float32)]
            four.append(jnp.concatenate(pair, axis=-1))
        turned = jnp.concatenate(four, axis=0).astype(BF16).T
        for k in range(2):
            parts = [turned[64 * k + 16 * d : 64 * k + 16 * d + 16] for d in range(4)]
            for q, part in enumerate(regroup(parts)):
                rows[b + q + 4 * k, 128:144, :] = part
    copies[3].wait()
    copies[4].wait()


def ready(latents, rotary, gain, key_up, value_up):
    b = latents.shape[0]
    return call(
        ready_kernel,
        (shape(b, 144, 128), shape(1024, 128)),
        (latents, rotary, gain.reshape(1, -1), key_up.reshape(512, 128), value_up.reshape(512, 128)),
        in_specs=whole(5, pltpu.HBM),
        limit=67043328,
        scratch=[
            VMEM(latents.shape, BF16),
            VMEM(rotary.shape, BF16),
            VMEM((1, 512), jnp.float32),
            pltpu.SemaphoreType.DMA((5,)),
        ],
    )


def expand_kernel(n, m, *refs):
    rows, heads, outs = refs[:n], refs[n : n + m], refs[n + m :]
    for i in range(n):
        a = rows[i]
        for g in range(a.shape[0] // 4):
            four = a[4 * g : 4 * g + 4]
            lhs = jnp.concatenate(
                [four[:, 32 * j : 32 * j + 32].reshape(128, 128) for j in range(4)], axis=-1
            )
            turned = jnp.concatenate(regroup([four[k, 128:144] for k in range(4)]), axis=0)
            for head, out in zip(heads, outs):
                w = jnp.concatenate([head[0:512, :], head[512:1024, :]], axis=-1)
                wide = jnp.dot(lhs, w, preferred_element_type=jnp.float32).astype(BF16)
                out[i, g, 0:4] = wide[:, 0:128].T.reshape(4, 32, 128)
                out[i, g, 4:6] = turned.reshape(2, 32, 128)
                out[i, g, 6:10] = wide[:, 128:256].reshape(4, 32, 128)


def expand(rows, heads):
    n, m, s = len(rows), len(heads), rows[0].shape[0]
    outs = call(
        functools.partial(expand_kernel, n, m),
        (shape(n, s // 4, 10, 32, 128),) * m,
        (*rows, *heads),
        limit=4 * MIB,
        flops=m * n * s * 32 * 512 * 256 * 2,
    )
    return list(outs)


def copier(copies, sems):
    def copy(src, dst):
        copies.append(pltpu.make_async_copy(src, dst, sems.at[len(copies)]))
        copies[-1].start()

    return copy


def spot(outer, inner, o, n):
    place = {outer: sender(outer, HOPS[o]), inner: sender(inner, HOPS[n])}
    return place["y"], place["x"]


def put_values(copy, values, unit, first, y, x):
    for g in range(unit.shape[0]):
        to = first + 4 * g
        rows = pl.ds(pl.multiple_of(x * 32, 32), 32)
        copy(unit.at[g, 6:10], values.at[to : to + 4, y, rows])


def line_keys(lined, sorted_, g):
    for y in range(SIDE):
        parts = [sorted_[y * SIDE + x, g] for x in range(SIDE)]
        for k, part in enumerate(regroup(parts)):
            lined[g, k, :, 128 * y : 128 * y + 128] = part


def sort_keys(sorted_, pieces, outer, inner):
    for o in range(len(HOPS)):
        mine = [pieces.pop(0) for _ in range(2 if o else 1)]
        units = [p.at[k] for p in mine for k in range(p.shape[0])]
        for n, unit in enumerate(units):
            y, x = spot(outer, inner, o, n)
            for g in range(sorted_.shape[1]):
                sorted_[y * SIDE + x, g] = unit[g, 0:6].reshape(192, 128)


def put_keys(copy, keys, lined, o, g):
    y = sender("y", HOPS[o])
    for k in range(4):
        lanes = pl.ds(pl.multiple_of((4 * g + k) * 512 + y * 128, 128), 128)
        copy(lined.at[k], keys.at[:, lanes])


def line_row(sorted_, lined, units, g):
    for n, unit in enumerate(units):
        sorted_[sender("x", HOPS[n])] = unit[g, 0:6].reshape(192, 128)
    for k, part in enumerate(regroup([sorted_[x] for x in range(SIDE)])):
        lined[k] = part


def early_kernel(*refs):
    pieces, (keys, values, sorted_, lined, sems) = list(refs[:8]), refs[8:]
    local = pieces[4]
    copies = []
    copy = copier(copies, sems)
    for h, (outer, inner) in enumerate(("xy", "yx")):
        first = (1 - h) * values.shape[0] // 2
        for o in range(4):
            piece = pieces.pop(0)
            for n in range(piece.shape[0]):
                put_values(copy, values, piece.at[n], first, *spot(outer, inner, o, n))
    for g in range(local.shape[1]):
        line_row(sorted_.at[g], lined.at[g], [local.at[n] for n in range(4)], g)
        put_keys(copy, keys, lined.at[g], 0, g)
    for each in copies:
        each.wait()


def line_kernel(*refs):
    pieces, lined, sorted_ = list(refs[:-2]), refs[-2], refs[-1]
    sort_keys(sorted_, pieces, "x", "y")
    for g in range(lined.shape[0]):
        line_keys(lined, sorted_, g)


def join_kernel(*refs):
    y_rest, x_pieces, y_lined = refs[:3], refs[3:9], refs[9]
    keys, values, sorted_, lined, sems = refs[12:]
    groups = y_lined.shape[0]
    copies = []
    copy = copier(copies, sems)
    for g in range(groups):
        for k in range(4):
            at = (4 * (groups + g) + k) * 512
            copy(y_lined.at[g, k], keys.at[:, at : at + 512])
    for (outer, inner), first, rest in (("xy", 4 * groups, y_rest), ("yx", 0, x_pieces[1::2])):
        for o, piece in enumerate(rest):
            for n in range(piece.shape[0]):
                put_values(copy, values, piece.at[n], first, *spot(outer, inner, o + 1, n + 1))
    for o in (3, 1, 2):
        own, rest = x_pieces[2 * o - 2], x_pieces[2 * o - 1]
        units = [own.at[0]] + [rest.at[n] for n in range(3)]
        for g in range(groups):
            line_row(sorted_.at[o - 1, g], lined.at[o - 1, g], units, g)
            put_keys(copy, keys, lined.at[o - 1, g], o, g)
    for each in copies:
        each.wait()


def finish(y_got, x_got):
    groups = y_got[0][0].shape[1]
    keys, values = shape(192, 2 * groups * 2048), shape(2 * groups * 4, SIDE, 128, 128)
    block = (groups, 4, 192, 128)
    sems = pltpu.SemaphoreType.DMA
    started = call(
        early_kernel,
        (keys, values),
        [p[0] for p in y_got + x_got],
        out_space=pltpu.HBM,
        limit=2 * MIB,
        scratch=[VMEM(block, BF16), VMEM(block, BF16), sems((groups * (14 + 4),))],
        nbytes=2 * MIB,
    )
    y_lined = call(
        line_kernel,
        shape(groups, 4, 192, 512),
        sum(y_got, []),
        limit=4 * MIB,
        scratch=[VMEM((SIDE * SIDE, groups, 192, 128), BF16)],
        nbytes=3 * MIB,
    )
    args = [p[1] for p in y_got[1:]] + sum(x_got[1:], []) + [y_lined, *started]
    return call(
        join_kernel,
        (keys, values),
        args,
        in_specs=whole(len(args) - 2) + whole(2, pltpu.HBM),
        out_space=pltpu.HBM,
        limit=6 * MIB,
        scratch=[VMEM((3, *block), BF16), VMEM((3, *block), BF16), sems((groups * (4 + 18 + 12),))],
        alias={len(args) - 2: 0, len(args) - 1: 1},
        nbytes=6 * MIB,
    )


def named_move(array, along, i, back=False):
    return move(array, along, -HOPS[i] if back else HOPS[i])


def shards(latents, rotary_rows, latent_gain, key_up, value_up):
    rows, head = ready(latents, rotary_rows, latent_gain, key_up, value_up)
    mine = lax.all_to_all(rows, "seq", split_axis=0, concat_axis=0, tiled=True)
    heads = {a: [head] + [named_move(head, a, i, back=True) for i in (1, 2, 3)] for a in "xy"}
    mine, heads["x"][1] = lax.optimization_barrier((mine, heads["x"][1]))
    half = mine.shape[0] // 2
    near = {"x": [mine[:half]], "y": [mine[half:]]}
    for i in (1, 2, 3):
        for a in "xy":
            near[a].append(named_move(near[a][0], a, i))
    got = {"x": [None] * 4, "y": [None] * 4}
    ahead = {"x": [None] * 4, "y": [None] * 4}
    for a in "yx":
        ahead[a][1:] = expand(near[a][:1], heads[OTHER[a]][1:])
    for i in (3, 1, 2):
        for a in "yx":
            ahead[a][i] = named_move(ahead[a][i], OTHER[a], i)
    for i in (3, 1, 2, 0):
        for a in "yx":
            (piece,) = expand(near[a][1:] if i else near[a], heads[OTHER[a]][i : i + 1])
            got[a][i] = [ahead[a][i], named_move(piece, OTHER[a], i)] if i else [piece]
    keys, values = finish(got["y"], got["x"])
    return keys[None, None], values.reshape(1, -1, 1, 128)


def solution(mesh):
    return jax.shard_map(
        shards,
        mesh=mesh,
        in_specs=(
            P(None, ("seq", "tp"), None),
            P(None, ("seq", "tp"), None),
            P(),
            P(None, "tp", None),
            P(None, "tp", None),
        ),
        out_specs=(P("seq", "tp", None, None), P("seq", None, "tp", None)),
        check_vma=False,
    )
```

```python
import functools

import jax
import jax.numpy as jnp
from jax import lax
from jax.experimental import pallas as pl
from jax.experimental.pallas import tpu as pltpu
from jax.sharding import PartitionSpec as P


SIDE = 4
HOPS = (0, 1, -1, 2)
VMEM = pltpu.VMEM
MIB = 1 << 20
BF16 = jnp.bfloat16
OTHER = {"x": "y", "y": "x"}


def move(array, along, hop):
    pairs = []
    for y in range(SIDE):
        for x in range(SIDE):
            to = (y, (x + hop) % SIDE) if along == "x" else ((y + hop) % SIDE, x)
            pairs.append((y * SIDE + x, to[0] * SIDE + to[1]))
    return lax.ppermute(array, "tp", pairs)


def sender(along, hop):
    t = lax.axis_index("tp")
    mine = t % SIDE if along == "x" else t // SIDE
    return (mine - hop + SIDE) % SIDE


def whole(n, space=VMEM):
    return [pl.BlockSpec(memory_space=space)] * n


def shape(*dims):
    return jax.ShapeDtypeStruct(dims, BF16)


def call(kernel, outs, args, out_space=VMEM, in_specs=None, limit=24 * MIB, scratch=(), alias=None, flops=0, nbytes=MIB):
    return pl.pallas_call(
        kernel,
        out_shape=outs,
        in_specs=in_specs or whole(len(args)),
        out_specs=jax.tree.map(lambda _: pl.BlockSpec(memory_space=out_space), outs),
        scratch_shapes=list(scratch),
        input_output_aliases=alias or {},
        compiler_params=pltpu.CompilerParams(vmem_limit_bytes=limit),
        cost_estimate=pl.CostEstimate(flops=flops, bytes_accessed=nbytes, transcendentals=0),
    )(*args)


def run_all(copies):
    for copy in copies:
        copy.start()
    for copy in copies:
        copy.wait()


def regroup(parts):
    return [jnp.concatenate([p[:, 32 * k : 32 * k + 32] for p in parts], axis=-1) for k in range(4)]


def ready_kernel(lat_in, rot_in, gain_in, rows, lat, rot, gain, sems):
    copies = [
        pltpu.make_async_copy(src, dst, sems.at[i])
        for i, (src, dst) in enumerate(
            (
                (lat_in, lat),
                (gain_in, gain),
                (rot_in, rot),
            )
        )
    ]
    for copy in copies:
        copy.start()
    copies[0].wait()
    copies[1].wait()
    gains = gain[...]
    for b in range(lat.shape[0]):
        v = lat[b].astype(jnp.float32)
        v = v * lax.rsqrt(jnp.mean(v * v, axis=-1, keepdims=True) + 1e-06) * gains
        v = v.astype(BF16)
        for j in range(4):
            rows[b, 32 * j : 32 * j + 32, :] = v[:, 128 * j : 128 * j + 128]
    copies[2].wait()
    for b in range(0, lat.shape[0], 8):
        four = []
        for q in range(4):
            pair = [rot[b + q].astype(jnp.float32), rot[b + q + 4].astype(jnp.float32)]
            four.append(jnp.concatenate(pair, axis=-1))
        turned = jnp.concatenate(four, axis=0).astype(BF16).T
        for k in range(2):
            parts = [turned[64 * k + 16 * d : 64 * k + 16 * d + 16] for d in range(4)]
            for q, part in enumerate(regroup(parts)):
                rows[b + q + 4 * k, 128:144, :] = part


def ready(latents, rotary, gain):
    b = latents.shape[0]
    return call(
        ready_kernel,
        shape(b, 144, 128),
        (latents, rotary, gain.reshape(1, -1)),
        in_specs=whole(3, pltpu.HBM),
        limit=67043328,
        scratch=[
            VMEM(latents.shape, BF16),
            VMEM(rotary.shape, BF16),
            VMEM((1, 512), jnp.float32),
            pltpu.SemaphoreType.DMA((3,)),
        ],
    )


def stack_kernel(key_in, value_in, after, weights, sems):
    del after
    run_all(
        [
            pltpu.make_async_copy(key_in, weights.at[0:512, :], sems.at[0]),
            pltpu.make_async_copy(value_in, weights.at[512:1024, :], sems.at[1]),
        ]
    )


def stack(key_up, value_up, after):
    return call(
        stack_kernel,
        shape(1024, 128),
        (key_up.reshape(512, 128), value_up.reshape(512, 128), after),
        in_specs=whole(3, pltpu.HBM),
        limit=60 * MIB,
        scratch=[pltpu.SemaphoreType.DMA((2,))],
    )


def expand_kernel(n, m, *refs):
    rows, heads, outs = refs[:n], refs[n : n + m], refs[n + m :]
    for i in range(n):
        a = rows[i]
        for g in range(a.shape[0] // 4):
            four = a[4 * g : 4 * g + 4]
            lhs = jnp.concatenate(
                [four[:, 32 * j : 32 * j + 32].reshape(128, 128) for j in range(4)], axis=-1
            )
            turned = jnp.concatenate(regroup([four[k, 128:144] for k in range(4)]), axis=0)
            for head, out in zip(heads, outs):
                w = jnp.concatenate([head[0:512, :], head[512:1024, :]], axis=-1)
                wide = jnp.dot(lhs, w, preferred_element_type=jnp.float32).astype(BF16)
                out[i, g, 0:4] = wide[:, 0:128].T.reshape(4, 32, 128)
                out[i, g, 4:6] = turned.reshape(2, 32, 128)
                out[i, g, 6:10] = wide[:, 128:256].reshape(4, 32, 128)


def expand(rows, heads):
    n, m, s = len(rows), len(heads), rows[0].shape[0]
    outs = call(
        functools.partial(expand_kernel, n, m),
        (shape(n, s // 4, 10, 32, 128),) * m,
        (*rows, *heads),
        limit=4 * MIB,
        flops=m * n * s * 32 * 512 * 256 * 2,
    )
    return list(outs)


def copier(copies, sems):
    def copy(src, dst):
        copies.append(pltpu.make_async_copy(src, dst, sems.at[len(copies)]))
        copies[-1].start()

    return copy


def spot(outer, inner, o, n):
    place = {outer: sender(outer, HOPS[o]), inner: sender(inner, HOPS[n])}
    return place["y"], place["x"]


def put_values(copy, values, unit, first, y, x):
    for g in range(unit.shape[0]):
        to = first + 4 * g
        rows = pl.ds(pl.multiple_of(x * 32, 32), 32)
        copy(unit.at[g, 6:10], values.at[to : to + 4, y, rows])


def line_keys(lined, sorted_, g):
    for y in range(SIDE):
        parts = [sorted_[y * SIDE + x, g] for x in range(SIDE)]
        for k, part in enumerate(regroup(parts)):
            lined[g, k, :, 128 * y : 128 * y + 128] = part


def sort_keys(sorted_, pieces, outer, inner):
    for o in range(len(HOPS)):
        mine = [pieces.pop(0) for _ in range(2 if o else 1)]
        units = [p.at[k] for p in mine for k in range(p.shape[0])]
        for n, unit in enumerate(units):
            y, x = spot(outer, inner, o, n)
            for g in range(sorted_.shape[1]):
                sorted_[y * SIDE + x, g] = unit[g, 0:6].reshape(192, 128)


def put_keys(copy, keys, lined, o, g):
    y = sender("y", HOPS[o])
    for k in range(4):
        lanes = pl.ds(pl.multiple_of((4 * g + k) * 512 + y * 128, 128), 128)
        copy(lined.at[k], keys.at[:, lanes])


def line_row(sorted_, lined, units, g):
    for n, unit in enumerate(units):
        sorted_[sender("x", HOPS[n])] = unit[g, 0:6].reshape(192, 128)
    for k, part in enumerate(regroup([sorted_[x] for x in range(SIDE)])):
        lined[k] = part


def early_kernel(*refs):
    pieces, (keys, values, sorted_, lined, sems) = list(refs[:8]), refs[8:]
    local = pieces[4]
    copies = []
    copy = copier(copies, sems)
    for h, (outer, inner) in enumerate(("xy", "yx")):
        first = (1 - h) * values.shape[0] // 2
        for o in range(4):
            piece = pieces.pop(0)
            for n in range(piece.shape[0]):
                put_values(copy, values, piece.at[n], first, *spot(outer, inner, o, n))
    for g in range(local.shape[1]):
        line_row(sorted_.at[g], lined.at[g], [local.at[n] for n in range(4)], g)
        put_keys(copy, keys, lined.at[g], 0, g)
    for each in copies:
        each.wait()


def line_kernel(*refs):
    pieces, lined, sorted_ = list(refs[:-2]), refs[-2], refs[-1]
    sort_keys(sorted_, pieces, "x", "y")
    for g in range(lined.shape[0]):
        line_keys(lined, sorted_, g)


def join_kernel(*refs):
    y_rest, x_pieces, y_lined = refs[:3], refs[3:9], refs[9]
    keys, values, sorted_, lined, sems = refs[12:]
    groups = y_lined.shape[0]
    copies = []
    copy = copier(copies, sems)
    for g in range(groups):
        for k in range(4):
            at = (4 * (groups + g) + k) * 512
            copy(y_lined.at[g, k], keys.at[:, at : at + 512])
    for (outer, inner), first, rest in (("xy", 4 * groups, y_rest), ("yx", 0, x_pieces[1::2])):
        for o, piece in enumerate(rest):
            for n in range(piece.shape[0]):
                put_values(copy, values, piece.at[n], first, *spot(outer, inner, o + 1, n + 1))
    for o in (3, 1, 2):
        own, rest = x_pieces[2 * o - 2], x_pieces[2 * o - 1]
        units = [own.at[0]] + [rest.at[n] for n in range(3)]
        for g in range(groups):
            line_row(sorted_.at[o - 1, g], lined.at[o - 1, g], units, g)
            put_keys(copy, keys, lined.at[o - 1, g], o, g)
    for each in copies:
        each.wait()


def finish(y_got, x_got):
    groups = y_got[0][0].shape[1]
    keys, values = shape(192, 2 * groups * 2048), shape(2 * groups * 4, SIDE, 128, 128)
    block = (groups, 4, 192, 128)
    sems = pltpu.SemaphoreType.DMA
    started = call(
        early_kernel,
        (keys, values),
        [p[0] for p in y_got + x_got],
        out_space=pltpu.HBM,
        limit=2 * MIB,
        scratch=[VMEM(block, BF16), VMEM(block, BF16), sems((groups * (14 + 4),))],
        nbytes=2 * MIB,
    )
    y_lined = call(
        line_kernel,
        shape(groups, 4, 192, 512),
        sum(y_got, []),
        limit=4 * MIB,
        scratch=[VMEM((SIDE * SIDE, groups, 192, 128), BF16)],
        nbytes=3 * MIB,
    )
    args = [p[1] for p in y_got[1:]] + sum(x_got[1:], []) + [y_lined, *started]
    return call(
        join_kernel,
        (keys, values),
        args,
        in_specs=whole(len(args) - 2) + whole(2, pltpu.HBM),
        out_space=pltpu.HBM,
        limit=6 * MIB,
        scratch=[VMEM((3, *block), BF16), VMEM((3, *block), BF16), sems((groups * (4 + 18 + 12),))],
        alias={len(args) - 2: 0, len(args) - 1: 1},
        nbytes=6 * MIB,
    )


def named_move(array, along, i, back=False):
    return move(array, along, -HOPS[i] if back else HOPS[i])


def shards(latents, rotary_rows, latent_gain, key_up, value_up):
    rows = ready(latents, rotary_rows, latent_gain)
    head = stack(key_up, value_up, rows)
    mine = lax.all_to_all(rows, "seq", split_axis=0, concat_axis=0, tiled=True)
    heads = {a: [head] + [named_move(head, a, i, back=True) for i in (1, 2, 3)] for a in "xy"}
    mine, heads["x"][1] = lax.optimization_barrier((mine, heads["x"][1]))
    half = mine.shape[0] // 2
    near = {"x": [mine[:half]], "y": [mine[half:]]}
    for i in (1, 2, 3):
        for a in "xy":
            near[a].append(named_move(near[a][0], a, i))
    got = {"x": [None] * 4, "y": [None] * 4}
    ahead = {"x": [None] * 4, "y": [None] * 4}
    for a in "yx":
        ahead[a][1:] = expand(near[a][:1], heads[OTHER[a]][1:])
    for i in (3, 1, 2):
        for a in "yx":
            ahead[a][i] = named_move(ahead[a][i], OTHER[a], i)
    for i in (3, 1, 2, 0):
        for a in "yx":
            (piece,) = expand(near[a][1:] if i else near[a], heads[OTHER[a]][i : i + 1])
            got[a][i] = [ahead[a][i], named_move(piece, OTHER[a], i)] if i else [piece]
    keys, values = finish(got["y"], got["x"])
    return keys[None, None], values.reshape(1, -1, 1, 128)


def solution(mesh):
    return jax.shard_map(
        shards,
        mesh=mesh,
        in_specs=(
            P(None, ("seq", "tp"), None),
            P(None, ("seq", "tp"), None),
            P(),
            P(None, "tp", None),
            P(None, "tp", None),
        ),
        out_specs=(P("seq", "tp", None, None), P("seq", None, "tp", None)),
        check_vma=False,
    )
```
